32 devices in a mesh: dp: 8 (over z, x), seq: 4 (over y, core).
Axes of the slice: x: 2, y: 2, z: 4, core: 2. Of those that a mesh axis runs over, the one named last changes fastest.
Arguments:
- tokens: bfloat16 [4608, 3584], P('dp'), may hold values from -6 to 6
- positions: int32 [3, 4608], P(None, 'dp'), may hold values from 0 to 2047
- loss_mask: int32 [4608], P('dp'), may hold values from 0 to 1, as said below
- sample_tokens: int32 [8, 3], replicated, may hold values from 96 to 384, as said below
- dest_slot: int32 [4608], P('dp'), may hold values from 0 to 6143, as said below
- norm_gain: float32 [3584], replicated, may hold values from 0.5 to 1.5
- q_weight: bfloat16 [3584, 2048], P(None, 'seq'), may hold values from -0.09375 to 0.09375
- k_weight: bfloat16 [3584, 512], P(None, 'seq'), may hold values from -0.09375 to 0.09375
- v_weight: bfloat16 [3584, 512], P(None, 'seq'), may hold values from -0.09375 to 0.09375
- q_bias: float32 [2048], P('seq'), may hold values from -3 to 3
- k_bias: float32 [512], P('seq'), may hold values from -3 to 3
- v_bias: float32 [512], P('seq'), may hold values from -3 to 3
- o_weight: bfloat16 [2048, 3584], P('seq'), may hold values from -0.125 to 0.125
Outputs:
- mixed: bfloat16 [6144, 3584], P(('dp', 'seq'))
- token_weight: float32 [6144], P(('dp', 'seq'))
The draws below stay inside these ranges and needn't reach their ends.
Inputs may be any that keep to these rules, and one draw needn't show every extreme that they name: `sample_tokens`: row r gives the token counts of the samples in the buckets of receiver r, of 384, 192 and 192 slots; each count lies between half of its bucket's slots and all of them. Some receiver has all three buckets full. All counts together equal the number of rows of tokens. `dest_slot`: every row has a slot of its own, and the slots that rows take are exactly the first sample_tokens[r, b] slots of each bucket b of each receiver r. Of the rows of one sender at most 96 go to one receiver; a receiver whose buckets are all full takes exactly 96 rows from every sender. `loss_mask`: the first of each sender's 576 rows is 1.
All inputs are finite; a program needn't handle non-finite values.
Results may differ from the reference program's by a relative error of at most 0.015.
Values may be sent and summed in bfloat16 or wider, within the bound.
A program may use at most 128 MiB of HBM per device.

```python
import math
import jax
import jax.numpy as jnp
from jax import lax

D = 3584
HQ = 16
KV = 4
DH = 128
BUCKET = 384
SRC = 576
N_DP = 8
N_SEQ = 4


def plan_tables(key):
    pairing_key = jax.random.fold_in(key, 11)
    length_key = jax.random.fold_in(key, 12)
    shuffle_key = jax.random.fold_in(key, 13)
    half_bucket = BUCKET // 2
    bucket_sizes = jnp.array([BUCKET, half_bucket, half_bucket], jnp.int32)
    pairing = jax.random.permutation(pairing_key, N_DP).astype(jnp.int32)
    pair_count = N_DP // 2
    first_lengths = jax.random.randint(length_key, (pair_count, 3), bucket_sizes // 2, bucket_sizes + 1).astype(jnp.int32)
    first_lengths = first_lengths.at[0].set(bucket_sizes)
    second_lengths = (3 * bucket_sizes // 2 - first_lengths).astype(jnp.int32)
    lengths = jnp.zeros((N_DP, 3), jnp.int32).at[pairing[0::2]].set(first_lengths).at[pairing[1::2]].set(second_lengths)
    local_slot = jnp.arange(2 * BUCKET, dtype=jnp.int32)
    bucket_id = (local_slot >= BUCKET).astype(jnp.int32) + (local_slot >= BUCKET + half_bucket).astype(jnp.int32)
    starts = jnp.array([0, BUCKET, BUCKET + half_bucket], jnp.int32)
    offset = local_slot - starts[bucket_id]
    filled = (offset[None, :] < lengths[:, bucket_id]).reshape(-1).astype(jnp.int32)
    order_index = (jnp.cumsum(filled) - 1).astype(jnp.int32)
    sender = order_index % N_DP
    within = jnp.clip(order_index // N_DP, 0, SRC - 1)
    sender_keys = jax.random.split(shuffle_key, N_DP)
    shuffles = jax.vmap(lambda one_key: jax.random.permutation(one_key, SRC))(sender_keys).astype(jnp.int32)
    source_row = (sender * SRC + shuffles[sender, within]).astype(jnp.int32)
    target = jnp.where(filled > 0, source_row, N_DP * SRC)
    global_slot = jnp.arange(N_DP * 2 * BUCKET, dtype=jnp.int32)
    dest = jnp.zeros((N_DP * SRC,), jnp.int32).at[target].set(global_slot, mode='drop')
    return (lengths, dest)


def draw_sample_tokens(key, part):
    return plan_tables(key)[0]


def draw_dest_slot(key, part):
    return plan_tables(key)[1]


def draw_loss_mask(key, part):
    row_total = N_DP * SRC
    row_ids = jnp.arange(row_total, dtype=jnp.int32)
    sender = row_ids // SRC
    level = jax.random.randint(jax.random.fold_in(key, 22), (), 15, 86).astype(jnp.int32)
    jitter = jax.random.randint(jax.random.fold_in(key, 23), (N_DP,), 50, 151).astype(jnp.int32)
    ramp = N_DP - 1 + 2 * sender
    threshold = level * ramp * jitter[sender]
    drawn = jax.random.randint(jax.random.fold_in(key, 21), (row_total,), 0, 100 * (3 * N_DP - 3) * 150)
    chosen = (drawn < threshold) | (row_ids % SRC == 0)
    return chosen.astype(jnp.int32)


def with_ends(values, key, low, high):
    dims = values.shape
    index_at = [jax.random.randint(jax.random.fold_in(key, axis), (), 0, dims[axis]) for axis in range(len(dims))]
    values = values.at[tuple(index_at)].set(low)
    longest = dims.index(max(dims))
    index_at[longest] = (index_at[longest] + 1) % dims[longest]
    return values.at[tuple(index_at)].set(high)


def block_levels(own_key, extent, shards, smallest, top_value):
    level, own = 1.0, jax.random.fold_in(own_key, 6)
    for position, parts in shards:
        draws = jnp.exp(jax.random.uniform(jax.random.fold_in(own, position), (parts,), jnp.float32, smallest / len(shards), top_value / len(shards)))
        level = level * jnp.repeat(draws, extent[position] // parts).reshape([-1 if axis == position else 1 for axis in range(len(extent))])
    return level


def bell_draw(own_key, shape, spread, bound, cuts=(), held_as=jnp.bfloat16):
    level = block_levels(own_key, shape, cuts, -0.22, 0.18) if cuts else 1.0
    entries = jax.random.normal(own_key, shape, jnp.float32) * spread * level
    return jnp.minimum(jnp.maximum(entries, -bound), bound).astype(held_as)


def setup_inputs(seed: int = 0) -> dict:
    streams_of = jax.random.split(jax.random.key(seed), 14)
    tokens = bell_draw(streams_of[0], (N_DP * SRC, D), 1.0, 6.0, ((0, 8),))
    positions = with_ends(jax.random.randint(streams_of[1], (3, N_DP * SRC), 0, 2048), jax.random.fold_in(streams_of[1], 1), 0, 2047).astype(jnp.int32)
    loss_mask = draw_loss_mask(jax.random.fold_in(streams_of[13], 71), 0)
    sample_tokens = draw_sample_tokens(jax.random.fold_in(streams_of[13], 71), 0)
    dest_slot = draw_dest_slot(jax.random.fold_in(streams_of[13], 71), 0)
    norm_gain = jnp.clip(1.0 + 0.1 * jax.random.normal(streams_of[5], (D,), jnp.float32), 0.5, 1.5)
    q_weight = bell_draw(streams_of[6], (D, HQ * DH), D ** -0.5, 0.09375, ((1, 4),))
    k_weight = bell_draw(streams_of[7], (D, KV * DH), D ** -0.5, 0.09375, ((1, 4),))
    v_weight = bell_draw(streams_of[8], (D, KV * DH), D ** -0.5, 0.09375, ((1, 4),))
    q_bias = bell_draw(streams_of[9], (HQ * DH,), 0.5, 3.0, ((0, 4),), jnp.float32)
    k_bias = bell_draw(streams_of[10], (KV * DH,), 0.5, 3.0, ((0, 4),), jnp.float32)
    v_bias = bell_draw(streams_of[11], (KV * DH,), 0.5, 3.0, ((0, 4),), jnp.float32)
    o_weight = bell_draw(streams_of[12], (HQ * DH, D), (HQ * DH) ** -0.5, 0.125, ((0, 4),))
    return {"tokens": tokens, "positions": positions, "loss_mask": loss_mask, "sample_tokens": sample_tokens, "dest_slot": dest_slot, "norm_gain": norm_gain, "q_weight": q_weight, "k_weight": k_weight, "v_weight": v_weight, "q_bias": q_bias, "k_bias": k_bias, "v_bias": v_bias, "o_weight": o_weight}


NORM_EPSILON = 1e-06
ROPE_BASE = 1000000.0

def rms_norm(rows_in, gain):
    widened = rows_in.astype(jnp.float32)
    mean_square = lax.optimization_barrier(jnp.mean(widened * widened, axis=-1, keepdims=True))
    return (widened * lax.rsqrt(mean_square + NORM_EPSILON) * gain).astype(jnp.bfloat16)

def rotary_tables(position_ids, head_size):
    half_size = head_size // 2
    pair_index = jnp.arange(half_size, dtype=jnp.int32)
    inv_freq = jnp.exp(pair_index.astype(jnp.float32) * (-2.0 * math.log(ROPE_BASE) / head_size))
    time_limit = head_size // 8
    height_limit = time_limit + 3 * head_size // 16
    chosen = jnp.where(pair_index[None, :] < time_limit, position_ids[0][:, None], jnp.where(pair_index[None, :] < height_limit, position_ids[1][:, None], position_ids[2][:, None]))
    angles = chosen.astype(jnp.float32) * inv_freq[None, :]
    return (jnp.cos(angles), jnp.sin(angles))

def rotate(heads_in, cosine, sine_part):
    half_size = heads_in.shape[-1] // 2
    first_half = heads_in[..., :half_size]
    second_half = heads_in[..., half_size:]
    cosine = cosine[:, None, :]
    sine_part = sine_part[:, None, :]
    return jnp.concatenate([first_half * cosine - second_half * sine_part, second_half * cosine + first_half * sine_part], axis=-1)

def attend_group(queries, key_rows, value_rows, lengths):
    block_count = queries.shape[0]
    row_count = queries.shape[1]
    scores = jnp.einsum('bqagd,bkad->bagqk', queries.astype(jnp.float32), key_rows.astype(jnp.float32)) * (1.0 / math.sqrt(DH))
    places = jnp.arange(row_count, dtype=jnp.int32)
    allowed = (places[:, None] >= places[None, :])[None] & (places[None, None, :] < lengths[:, None, None])
    scores = jnp.where(allowed[:, None, None], scores, -1e+30)
    weights = jax.nn.softmax(scores, axis=-1).astype(jnp.bfloat16)
    context = jnp.einsum('bagqk,bkad->bqagd', weights.astype(jnp.float32), value_rows.astype(jnp.float32))
    live_rows = places[None, :] < lengths[:, None]
    context = jnp.where(live_rows[:, :, None, None, None], context, 0.0).astype(jnp.bfloat16)
    return context.reshape(block_count * row_count, -1)

def attend_buckets(q_rows, k_rows, v_rows, lengths, kv_count, group_size):
    half_bucket = BUCKET // 2
    first_part = attend_group(q_rows[:BUCKET].reshape(1, BUCKET, kv_count, group_size, DH), k_rows[:BUCKET].reshape(1, BUCKET, kv_count, DH), v_rows[:BUCKET].reshape(1, BUCKET, kv_count, DH), lengths[:1])
    second_part = attend_group(q_rows[BUCKET:].reshape(2, half_bucket, kv_count, group_size, DH), k_rows[BUCKET:].reshape(2, half_bucket, kv_count, DH), v_rows[BUCKET:].reshape(2, half_bucket, kv_count, DH), lengths[1:])
    return jnp.concatenate([first_part, second_part], axis=0)

def reference(tokens, positions, loss_mask, sample_tokens, dest_slot, norm_gain, q_weight, k_weight, v_weight, q_bias, k_bias, v_bias, o_weight):
    peer_count = sample_tokens.shape[0]
    slot_count = 2 * BUCKET
    total_slots = peer_count * slot_count
    head_count = q_weight.shape[1] // DH
    kv_count = k_weight.shape[1] // DH
    group_size = head_count // kv_count
    normed = rms_norm(tokens, norm_gain)
    queries = (jnp.dot(normed, q_weight, preferred_element_type=jnp.float32) + q_bias).astype(jnp.bfloat16)
    key_rows = (jnp.dot(normed, k_weight, preferred_element_type=jnp.float32) + k_bias).astype(jnp.bfloat16)
    value_rows = (jnp.dot(normed, v_weight, preferred_element_type=jnp.float32) + v_bias).astype(jnp.bfloat16)
    cosine, sine_part = rotary_tables(positions, DH)
    queries = rotate(queries.astype(jnp.float32).reshape(-1, head_count, DH), cosine, sine_part).astype(jnp.bfloat16)
    key_rows = rotate(key_rows.astype(jnp.float32).reshape(-1, kv_count, DH), cosine, sine_part).astype(jnp.bfloat16)
    q_slots = jnp.zeros((total_slots, head_count * DH), jnp.bfloat16).at[dest_slot].set(queries.reshape(-1, head_count * DH))
    k_slots = jnp.zeros((total_slots, kv_count * DH), jnp.bfloat16).at[dest_slot].set(key_rows.reshape(-1, kv_count * DH))
    v_slots = jnp.zeros((total_slots, kv_count * DH), jnp.bfloat16).at[dest_slot].set(value_rows)

    def attend(inputs):
        q_rows, k_rows, v_rows, lengths = inputs
        return attend_buckets(q_rows, k_rows, v_rows, lengths, kv_count, group_size)
    context = lax.map(attend, (q_slots.reshape(peer_count, slot_count, head_count * DH), k_slots.reshape(peer_count, slot_count, kv_count * DH), v_slots.reshape(peer_count, slot_count, kv_count * DH), sample_tokens))
    context = context.reshape(total_slots, head_count * DH)
    slice_width = head_count * DH // N_SEQ
    head_total = jnp.zeros((total_slots, tokens.shape[1]), jnp.float32)
    for group_index in range(N_SEQ):
        partial_value = jnp.dot(context[:, group_index * slice_width:(group_index + 1) * slice_width], o_weight[group_index * slice_width:(group_index + 1) * slice_width], preferred_element_type=jnp.float32).astype(jnp.bfloat16)
        head_total = head_total + partial_value.astype(jnp.float32)
    mixed = head_total.astype(jnp.bfloat16)
    mask_float = loss_mask.astype(jnp.float32)
    token_count = jnp.sum(mask_float)
    row_scale = tokens.shape[0] / token_count
    token_weight = jnp.zeros((total_slots,), jnp.float32).at[dest_slot].set(mask_float * row_scale)
    return (mixed, token_weight)
```

```python
import functools
import math

import jax
import jax.numpy as jnp
import numpy as np
from jax import lax
from jax.experimental import pallas as pl
from jax.experimental.pallas import tpu as pltpu
from jax.sharding import PartitionSpec as P

DH = 128
BUCKET = 384
LANES = 128
PIECE = 256
QUADS, X_PAIRS, Z_PAIRS = 1, 2, 1
VMEM_LIMIT = 65000000

NORM_EPSILON = 1e-06
ROPE_BASE = 1000000.0
F32 = jnp.float32
BF16 = jnp.bfloat16


def iota(shape, axis):
    return lax.broadcasted_iota(jnp.int32, shape, axis)


HIGH, LOW = 64, 32
HIGH_ROWS, LOW_ROWS = 256, 128


def turn_tables():
    half_size = DH // 2
    pair = np.arange(half_size, dtype=np.float32)
    freq = np.exp(pair * np.float32(-2.0 * math.log(ROPE_BASE) / DH)).astype(np.float64)
    time_limit = DH // 8
    height_limit = time_limit + 3 * DH // 16
    axis_of = np.where(pair < time_limit, 0, np.where(pair < height_limit, 1, 2))
    sign = np.concatenate([-np.ones(half_size), np.ones(half_size)])
    blocks = []
    for count, step, rows in ((HIGH, LOW, HIGH_ROWS), (LOW, 1, LOW_ROWS)):
        table = np.zeros((rows, 2 * DH))
        for axis in range(3):
            angles = np.arange(count)[:, None] * float(step) * freq[None, :]
            chosen = (axis_of == axis)[None, :]
            cos = np.where(chosen, np.cos(angles), 0.0)
            sin = np.where(chosen, np.sin(angles), 0.0)
            at = slice(axis * count, (axis + 1) * count)
            table[at, :DH] = np.concatenate([cos, cos], axis=1)
            table[at, DH:] = np.concatenate([sin, sin], axis=1) * sign[None, :]
        top = table.astype(jnp.bfloat16)
        rest = (table - top.astype(np.float64)).astype(jnp.bfloat16)
        blocks += [top, rest]
    return np.concatenate(blocks, axis=0)


def rotary_tables(pos_ref, table, cos_out, sin_out):
    ids = pos_ref[...]
    rows = ids.shape[1]
    high = ids // LOW
    low = ids - high * LOW
    kind = iota((8, rows), 0)
    split = jnp.zeros((8, rows), jnp.int32)
    for axis in range(3):
        split = jnp.where(kind == 2 * axis, high[axis : axis + 1], split)
        split = jnp.where(kind == 2 * axis + 1, low[axis : axis + 1], split)
    width = HIGH_ROWS + LOW_ROWS
    column, row = iota((8, width), 1), iota((8, width), 0)
    low_at = column - HIGH_ROWS
    wanted = jnp.where(column < HIGH_ROWS, 2 * (column // HIGH), 2 * (low_at // LOW) + 1)
    spread = jnp.where(row == wanted, 1.0, 0.0).astype(BF16)
    told = lax.dot_general(
        split.astype(F32).astype(BF16), spread, (((0,), (0,)), ((), ())),
        preferred_element_type=F32,
    )
    at = iota((1, width), 1)
    value = jnp.where(
        at < HIGH_ROWS,
        jnp.where(at < 3 * HIGH, at % HIGH, -1),
        jnp.where(at < HIGH_ROWS + 3 * LOW, (at - HIGH_ROWS) % LOW, -1),
    ).astype(F32)
    hot = jnp.where(told == value, 1.0, 0.0).astype(BF16)
    hot_high, hot_low = hot[:, :HIGH_ROWS], hot[:, HIGH_ROWS:]
    low_from = 2 * HIGH_ROWS

    def look(one, first, count):
        return jnp.dot(one, table[first : first + count], preferred_element_type=F32) + jnp.dot(
            one, table[first + count : first + 2 * count], preferred_element_type=F32
        )

    big = look(hot_high, 0, HIGH_ROWS)
    small = look(hot_low, low_from, LOW_ROWS)
    cos_out[...] = big[:, :DH] * small[:, :DH] - big[:, DH:] * small[:, DH:]
    sin_out[...] = big[:, DH:] * small[:, :DH] + big[:, :DH] * small[:, DH:]


def pack_plan(peers, slot_count, group, slot_ref, mask_ref, select_out, info_out):
    rows = slot_ref.shape[0]
    slots = slot_ref[...][None, :]
    peer = slots // slot_count
    local = slots - peer * slot_count + 1
    mask = mask_ref[...][None, :].astype(F32)
    mask_sum = jnp.sum(mask, axis=1, keepdims=True)
    hot = jnp.where(iota((peers, rows), 0) == peer, 1.0, 0.0)
    earlier = jnp.where(iota((rows, rows), 0) < iota((rows, rows), 1), 1.0, 0.0).astype(BF16)
    counts = jnp.dot(hot.astype(BF16), earlier, preferred_element_type=F32)
    rank = jnp.sum(hot * counts, axis=0, keepdims=True).astype(jnp.int32)
    place = peer * LANES + rank
    high = local // 32
    kind = iota((8, rows), 0)
    facts = jnp.where(
        kind == 0,
        high.astype(F32),
        jnp.where(kind == 1, (local - high * 32).astype(F32), jnp.where(kind == 2, mask, 0.0)),
    ).astype(BF16)
    span = group * LANES
    for g in range(peers // group):
        select = jnp.where(iota((span, rows), 0) + g * span == place, 1.0, 0.0).astype(BF16)
        select_out[g * span : (g + 1) * span, :] = select
        told = lax.dot_general(facts, select, (((1,), (1,)), ((), ())), preferred_element_type=F32)
        told = jnp.where(iota(told.shape, 0) == 3, mask_sum, told)
        for p in range(group):
            info_out[g * group + p] = told[:, p * LANES : (p + 1) * LANES]


def attend(q_slots, kv_slots, lengths, heads, per_kv, kv_count, ctx):
    start = 0
    scale = 1.0 / math.sqrt(DH)
    for size, length in zip((BUCKET, BUCKET // 2, BUCKET // 2), lengths):
        rows = slice(start, start + size)
        q_at, k_at = iota((size, size), 0), iota((size, size), 1)
        allowed = (q_at >= k_at) & (k_at < length)
        live = iota((size, DH), 0) < length
        for h in heads:
            pair = h // per_kv
            key = kv_slots[rows, pair * DH : (pair + 1) * DH]
            value = kv_slots[rows, (kv_count + pair) * DH : (kv_count + pair + 1) * DH]
            cols = slice(h * DH, (h + 1) * DH)
            scores = lax.dot_general(
                q_slots[rows, cols], key, (((1,), (1,)), ((), ())), preferred_element_type=F32
            )
            scores = jnp.where(allowed, scores * scale, -1e30)
            top = jnp.max(scores, axis=1, keepdims=True)
            weights = jnp.exp(scores - top)
            total = jnp.sum(weights, axis=1, keepdims=True)
            out = jnp.dot(weights.astype(BF16), value, preferred_element_type=F32) / total
            ctx[rows, cols] = jnp.where(live, out, 0.0).astype(BF16)
        start += size


def layer_kernel(
    peers, group, seq_count, q_heads, kv_heads, chunk, room, strips, pieces,
    tok_hbm, gain_ref, qw_hbm, kw_hbm, vw_hbm, qb_ref, kb_ref, vb_ref, pos_ref,
    slot_ref, mask_ref, ow_hbm, table_hbm,
    mixed_ref, weight_ref,
    x, squares, qw, kvw, ow, table, pick, told_out, got_info, q_out, q_got, kv_out, kv_got,
    select, padded, q_slots, kv_slots, ctx, ctx_far, w_far, held, pair, pair_in,
    far_pair, near_in, far_out, far_in, cos_ref, sin_ref,
    data_send, data_recv, info_send, info_recv, near_send, near_recv,
    pair_send, pair_recv, far_send, far_recv, load_sem,
    y_send, y_recv, x_send, x_recv, z_send, z_recv, ctx_send, ctx_recv,
):
    me = lax.axis_index("dp")
    seat = lax.axis_index("seq")
    half = seat // 2
    core = seat % 2
    partner = half * 2 + (1 - core)
    across = (1 - half) * 2 + core
    a = me % 2
    b = (me // 2) % 2
    x_peer = me + 1 - 2 * a
    z_peer = me + 2 - 4 * b
    q_stages = q_out.shape[0]
    per_stage = q_heads // q_stages
    rows, depth = x.shape
    slot_count = q_slots.shape[0]
    part = slot_count // seq_count
    block_rows = 2 * part
    wide_cols = pieces * PIECE
    out_width = ow.shape[1]
    chunks = (out_width - wide_cols) // chunk
    strip = rows // strips
    kv_cols = kv_heads * DH

    barrier = pltpu.get_barrier_semaphore()
    for d in range(1, peers):
        pl.semaphore_signal(barrier, inc=1, device_id={"dp": (me + d) % peers})
    pl.semaphore_signal(barrier, inc=1, device_id={"seq": partner})
    pl.semaphore_signal(barrier, inc=1, device_id={"seq": across})
    token_loads = [
        pltpu.make_async_copy(
            tok_hbm.at[i * strip : (i + 1) * strip], x.at[i * strip : (i + 1) * strip],
            load_sem.at[i],
        )
        for i in range(strips)
    ]
    k_load = pltpu.make_async_copy(kw_hbm, kvw.at[:, :kv_cols], load_sem.at[strips])
    v_load = pltpu.make_async_copy(vw_hbm, kvw.at[:, kv_cols:], load_sem.at[strips + 1])
    q_load = pltpu.make_async_copy(qw_hbm, qw, load_sem.at[strips + 2])
    o_load = pltpu.make_async_copy(ow_hbm, ow, load_sem.at[strips + 3])
    table_load = pltpu.make_async_copy(table_hbm, table, load_sem.at[strips + 4])
    for copy in [table_load] + token_loads + [k_load, v_load, q_load, o_load]:
        copy.start()

    y_own, x_jobs, z_jobs = [], [], []
    for k in range(QUADS):
        own = 4 * k + 2 * b + a
        y_at = len(y_own)
        y_own.append(own)
        z_at = len(z_jobs)
        z_jobs.append((own, y_at))
        x_jobs.append((own, "y", y_at))
        x_jobs.append((4 * k + 2 * (1 - b) + a, "z", z_at))
    for k in range(X_PAIRS):
        own = 4 * QUADS + 2 * k + a
        x_jobs.append((own, "y", len(y_own)))
        y_own.append(own)
    for k in range(Z_PAIRS):
        own = 4 * QUADS + 2 * X_PAIRS + 2 * k + b
        z_jobs.append((own, len(y_own)))
        y_own.append(own)

    def y_copy(i):
        at = pl.multiple_of(y_own[i] * PIECE, PIECE)
        return pltpu.make_async_remote_copy(
            ow_hbm.at[:, pl.ds(at, PIECE)], w_far.at[y_own[i]], y_send.at[i], y_recv.at[i],
            device_id={"seq": across},
        )

    def x_copy(i):
        own = x_jobs[i][0]
        return pltpu.make_async_remote_copy(
            w_far.at[own], w_far.at[own], x_send.at[i], x_recv.at[i], device_id={"dp": x_peer}
        )

    def z_copy(i):
        own = z_jobs[i][0]
        return pltpu.make_async_remote_copy(
            w_far.at[own], w_far.at[own], z_send.at[i], z_recv.at[i], device_id={"dp": z_peer}
        )

    def from_y(i):
        y_copy(i).wait_recv()
        for n, (_, source, at) in enumerate(x_jobs):
            if source == "y" and at == i:
                x_copy(n).start()
        for n, (_, at) in enumerate(z_jobs):
            if at == i:
                z_copy(n).start()

    def from_z(i):
        z_copy(i).wait_recv()
        for n, (_, source, at) in enumerate(x_jobs):
            if source == "z" and at == i:
                x_copy(n).start()

    pack_plan(peers, slot_count, group, slot_ref, mask_ref, pick, told_out)
    gain = gain_ref[...][None, :]
    for i in range(strips):
        token_loads[i].wait()
        at = slice(i * strip, (i + 1) * strip)
        total = jnp.zeros((strip, LANES), F32)
        for c in range(depth // LANES):
            cols = slice(c * LANES, (c + 1) * LANES)
            entry = x[at, cols].astype(F32)
            total = total + entry * entry
            x[at, cols] = (entry * gain[:, cols]).astype(BF16)
        squares[at, :] = jnp.sum(total, axis=1, keepdims=True)
    inverse = lax.rsqrt(squares[...] * (1.0 / depth) + NORM_EPSILON)

    def info_copy(d):
        to = (me + d) % peers
        return pltpu.make_async_remote_copy(
            told_out.at[to], got_info.at[me], info_send.at[d], info_recv.at[d],
            device_id={"dp": to},
        )

    def ctx_copy(stage):
        cols = slice(stage * per_stage * DH, (stage + 1) * per_stage * DH)
        return pltpu.make_async_remote_copy(
            ctx.at[pl.ds(pl.multiple_of((1 - half) * block_rows, block_rows), block_rows), cols],
            ctx_far.at[:, cols], ctx_send.at[stage], ctx_recv.at[stage],
            device_id={"seq": across},
        )

    def data_copy(stage, d):
        to = (me + d) % peers
        source, target = (kv_out, kv_got) if stage == 0 else (q_out, q_got)
        if stage > 0:
            source, target = source.at[stage - 1], target.at[stage - 1]
        return pltpu.make_async_remote_copy(
            source.at[to], target.at[me], data_send.at[stage, d], data_recv.at[stage, d],
            device_id={"dp": to},
        )

    def turn(wide):
        return wide * cos_ref[...] + pltpu.roll(wide, DH // 2, 1) * sin_ref[...]

    def pack(stage, values):
        span = group * LANES
        target, kept = (kv_out, kv_got) if stage == 0 else (q_out, q_got)
        if stage > 0:
            target, kept = target.at[stage - 1], kept.at[stage - 1]
        for g in range(peers // group):
            moved = jnp.dot(
                pick[g * span : (g + 1) * span, :], values, preferred_element_type=F32
            ).astype(BF16)
            for p in range(group):
                target[g * group + p] = moved[p * LANES : p * LANES + room]
        for d in range(1, peers):
            data_copy(stage, d).start()
        kept[me] = target[me]

    pl.semaphore_wait(barrier, peers + 1)
    for i in range(len(y_own)):
        y_copy(i).start()
    for d in range(1, peers):
        info_copy(d).start()
    got_info[me] = told_out[me]
    table_load.wait()
    rotary_tables(pos_ref, table, cos_ref, sin_ref)
    k_load.wait()
    v_load.wait()
    product = jnp.dot(x[...], kvw[...], preferred_element_type=F32)
    heads_out = []
    for h in range(2 * kv_heads):
        bias_ref, at = (kb_ref, h) if h < kv_heads else (vb_ref, h - kv_heads)
        bias = bias_ref[at * DH : (at + 1) * DH][None, :]
        head = (product[:, h * DH : (h + 1) * DH] * inverse + bias).astype(BF16)
        if h < kv_heads:
            head = turn(head.astype(F32)).astype(BF16)
        heads_out.append(head)
    pack(0, jnp.concatenate(heads_out, axis=1))
    q_load.wait()
    for stage in range(q_stages):
        cols = slice(stage * per_stage * DH, (stage + 1) * per_stage * DH)
        product = jnp.dot(x[...], qw[:, cols], preferred_element_type=F32)
        heads_out = []
        for i in range(per_stage):
            h = stage * per_stage + i
            bias = qb_ref[h * DH : (h + 1) * DH][None, :]
            head = (product[:, i * DH : (i + 1) * DH] * inverse + bias).astype(BF16)
            heads_out.append(turn(head.astype(F32)).astype(BF16))
        pack(stage + 1, jnp.concatenate(heads_out, axis=1))

    padded[...] = jnp.zeros_like(padded)
    for d in range(1, peers):
        info_copy(d).wait()
    count = jnp.zeros((1, LANES), F32)
    slot_at = iota((slot_count, LANES), 0).astype(F32)
    facts = []
    filled = [jnp.zeros((1, LANES), F32) for _ in range(3)]
    starts = (0, BUCKET, BUCKET + BUCKET // 2, 2 * BUCKET)
    for p in range(peers):
        told = got_info[p]
        facts.append(told)
        count = count + told[3:4]
        local = told[0:1] * 32.0 + told[1:2] - 1.0
        for bucket in range(3):
            inside = (local >= float(starts[bucket])) & (local < float(starts[bucket + 1]))
            filled[bucket] = filled[bucket] + jnp.where(inside, 1.0, 0.0)
        select[:, p * LANES : (p + 1) * LANES] = jnp.where(slot_at == local, 1.0, 0.0).astype(BF16)
    flags = jnp.concatenate(facts, axis=1).astype(BF16)
    own_select = select[pl.ds(pl.multiple_of(seat * part, part), part), :]
    seen = lax.dot_general(flags, own_select, (((1,), (1,)), ((), ())), preferred_element_type=F32)
    weight_ref[...] = seen[2:3] * ((peers * rows) / count[:, :1])

    def place(stage):
        for d in range(1, peers):
            data_copy(stage, d).wait()
        source = kv_got if stage == 0 else q_got.at[stage - 1]
        width = source.shape[2]
        for p in range(peers):
            padded[p * LANES : p * LANES + room, :width] = source[p]
        return jnp.dot(select[...], padded[:, :width], preferred_element_type=F32).astype(BF16)

    lengths = [jnp.sum(one, axis=1, keepdims=True).astype(jnp.int32) for one in filled]
    y_next = 0
    z_next = 0
    y_count, z_count = len(y_own), len(z_jobs)
    steps = q_stages + 1
    for stage in range(steps):
        while y_next < (stage + 1) * y_count // steps:
            from_y(y_next)
            y_next += 1
        if stage == 0:
            kv_slots[...] = place(0)
            continue
        while z_next < (stage * QUADS) // q_stages:
            from_z(z_next)
            z_next += 1
        q_at = stage - 1
        cols = slice(q_at * per_stage * DH, (q_at + 1) * per_stage * DH)
        q_slots[:, cols] = place(stage)
        heads = range(q_at * per_stage, (q_at + 1) * per_stage)
        attend(q_slots, kv_slots, lengths, heads, q_heads // kv_heads, kv_heads, ctx)
        ctx_copy(q_at).start()
    o_load.wait()

    def near_copy(j):
        to_row = pl.multiple_of((1 - core) * part, part)
        cols = slice(j * chunk, (j + 1) * chunk)
        return pltpu.make_async_remote_copy(
            far_pair.at[pl.ds(to_row, part), cols], near_in.at[:, cols],
            near_send.at[j], near_recv.at[j], device_id={"seq": partner},
        )

    def far_copy(j):
        cols = slice(j * chunk, (j + 1) * chunk)
        return pltpu.make_async_remote_copy(
            far_out.at[:, cols], far_in.at[:, cols], far_send.at[j], far_recv.at[j],
            device_id={"seq": across},
        )

    groups = [(i * PIECE, PIECE) for i in range(pieces)]
    groups += [(wide_cols + j * chunk, chunk) for j in range(chunks)]

    def pair_copy(n):
        first, width = groups[n]
        to_row = pl.multiple_of((1 - core) * part, part)
        return pltpu.make_async_remote_copy(
            pair.at[pl.ds(to_row, part), first : first + width],
            pair_in.at[:, first : first + width],
            pair_send.at[n], pair_recv.at[n], device_id={"seq": partner},
        )

    mine_at = pl.multiple_of(half * block_rows, block_rows)
    far_at = pl.multiple_of((1 - half) * block_rows, block_rows)
    own_at = pl.multiple_of(core * part, part)

    def forward(j):
        near_copy(j).wait_recv()
        cols = slice(j * chunk, (j + 1) * chunk)
        kept = far_pair[pl.ds(own_at, part), cols].astype(F32)
        far_out[:, cols] = (kept + near_in[:, cols].astype(F32)).astype(BF16)
        far_copy(j).start()

    for j in range(chunks):
        cols = slice(j * chunk, (j + 1) * chunk)
        w = ow[:, wide_cols + j * chunk : wide_cols + (j + 1) * chunk]
        far_pair[:, cols] = jnp.dot(
            ctx[pl.ds(far_at, block_rows), :], w, preferred_element_type=F32
        ).astype(BF16)
        near_copy(j).start()
        if j > 0:
            forward(j - 1)
    if chunks:
        forward(chunks - 1)
    for j in range(chunks):
        first, width = groups[pieces + j]
        pair[:, first : first + width] = jnp.dot(
            ctx[pl.ds(mine_at, block_rows), :], ow[:, first : first + width],
            preferred_element_type=F32,
        ).astype(BF16)
        pair_copy(pieces + j).start()
    for i in range(pieces):
        held[:, i * PIECE : (i + 1) * PIECE] = jnp.dot(
            ctx[pl.ds(mine_at, block_rows), :], ow[:, i * PIECE : (i + 1) * PIECE],
            preferred_element_type=F32,
        )
    for stage in range(q_stages):
        ctx_copy(stage).wait()
    for i in range(y_count):
        y_copy(i).wait_send()

    def finish(i):
        cols = slice(i * PIECE, (i + 1) * PIECE)
        pair[:, cols] = (
            held[:, cols] + jnp.dot(ctx_far[...], w_far[i], preferred_element_type=F32)
        ).astype(BF16)
        pair_copy(i).start()

    for k in range(X_PAIRS):
        x_copy(2 * QUADS + k).wait()
        finish(4 * QUADS + 2 * k)
        finish(4 * QUADS + 2 * k + 1)
    for k in range(Z_PAIRS):
        z_copy(QUADS + k).wait()
        finish(4 * QUADS + 2 * X_PAIRS + 2 * k)
        finish(4 * QUADS + 2 * X_PAIRS + 2 * k + 1)
    for k in range(QUADS):
        z_copy(k).wait_send()
        x_copy(2 * k).wait()
        x_copy(2 * k + 1).wait()
        for i in range(4 * k, 4 * k + 4):
            finish(i)
    for n in list(range(pieces, pieces + chunks)) + list(range(pieces)):
        first, width = groups[n]
        cols = slice(first, first + width)
        pair_copy(n).wait()
        total = pair[pl.ds(own_at, part), cols].astype(F32) + pair_in[:, cols].astype(F32)
        if n >= pieces:
            j = n - pieces
            near_copy(j).wait_send()
            far_copy(j).wait()
            total = total + far_in[:, j * chunk : (j + 1) * chunk].astype(F32)
        mixed_ref[:, cols] = total.astype(BF16)


def deliver(mixed_in, weight_in, mixed_hbm, weight_hbm, flat, sems):
    big = pltpu.make_async_copy(mixed_in, mixed_hbm, sems.at[0])
    big.start()
    flat[...] = weight_in[0, :]
    small = pltpu.make_async_copy(flat, weight_hbm, sems.at[1])
    small.start()
    big.wait()
    small.wait()


def per_device(
    tokens, positions, loss_mask, sample_tokens, dest_slot, norm_gain,
    q_weight, k_weight, v_weight, q_bias, k_bias, v_bias, o_weight,
):
    peers = lax.axis_size("dp")
    seq_count = lax.axis_size("seq")
    rows, depth = tokens.shape
    slot_count = 2 * BUCKET
    room = -(-(slot_count // peers) // 16) * 16
    group = math.gcd(peers, 8)
    q_heads = q_weight.shape[1] // DH
    kv_heads = k_weight.shape[1] // DH
    per_stage = math.gcd(q_heads, 2)
    stages = q_heads // per_stage
    strips = math.gcd(rows // 16, 4)
    part = slot_count // seq_count
    out_width = o_weight.shape[1]
    pieces = 4 * QUADS + 2 * X_PAIRS + 2 * Z_PAIRS
    wide_cols = pieces * PIECE
    narrow = out_width - wide_cols
    chunk = math.gcd(narrow, 512)
    chunks = narrow // chunk
    kv_width = 2 * kv_heads * DH
    q_width = per_stage * DH
    y_count = QUADS + X_PAIRS + Z_PAIRS
    x_count = 2 * QUADS + X_PAIRS
    z_count = QUADS + Z_PAIRS
    vmem = pl.BlockSpec(memory_space=pltpu.VMEM)
    hbm = pl.BlockSpec(memory_space=pl.ANY)
    dma = pltpu.SemaphoreType.DMA
    table = turn_tables()
    mixed, weight = pl.pallas_call(
        functools.partial(
            layer_kernel, peers, group, seq_count, q_heads, kv_heads, chunk, room, strips, pieces
        ),
        in_specs=[
            hbm, vmem, hbm, hbm, hbm, vmem, vmem, vmem, vmem, vmem, vmem, hbm, hbm,
        ],
        out_specs=[vmem, vmem],
        out_shape=[
            jax.ShapeDtypeStruct((part, out_width), BF16),
            jax.ShapeDtypeStruct((1, part), F32),
        ],
        scratch_shapes=[
            pltpu.VMEM((rows, depth), BF16),
            pltpu.VMEM((rows, 1), F32),
            pltpu.VMEM(q_weight.shape, BF16),
            pltpu.VMEM((depth, kv_width), BF16),
            pltpu.VMEM(o_weight.shape, BF16),
            pltpu.VMEM(table.shape, BF16),
            pltpu.VMEM((peers * LANES, rows), BF16),
            pltpu.VMEM((peers, 8, LANES), F32),
            pltpu.VMEM((peers, 8, LANES), F32),
            pltpu.VMEM((stages, peers, room, q_width), BF16),
            pltpu.VMEM((stages, peers, room, q_width), BF16),
            pltpu.VMEM((peers, room, kv_width), BF16),
            pltpu.VMEM((peers, room, kv_width), BF16),
            pltpu.VMEM((slot_count, peers * LANES), BF16),
            pltpu.VMEM((peers * LANES, max(kv_width, q_width)), BF16),
            pltpu.VMEM((slot_count, q_heads * DH), BF16),
            pltpu.VMEM((slot_count, kv_width), BF16),
            pltpu.VMEM((slot_count, q_heads * DH), BF16),
            pltpu.VMEM((2 * part, q_heads * DH), BF16),
            pltpu.VMEM((pieces, o_weight.shape[0], PIECE), BF16),
            pltpu.VMEM((2 * part, wide_cols), F32),
            pltpu.VMEM((2 * part, out_width), BF16),
            pltpu.VMEM((part, out_width), BF16),
            pltpu.VMEM((2 * part, narrow), BF16),
            pltpu.VMEM((part, narrow), BF16),
            pltpu.VMEM((part, narrow), BF16),
            pltpu.VMEM((part, narrow), BF16),
            pltpu.VMEM((rows, DH), F32),
            pltpu.VMEM((rows, DH), F32),
            dma((stages + 1, peers)), dma((stages + 1, peers)), dma((peers,)), dma((peers,)),
            dma((chunks,)), dma((chunks,)), dma((pieces + chunks,)), dma((pieces + chunks,)),
            dma((chunks,)), dma((chunks,)), dma((strips + 5,)),
            dma((y_count,)), dma((y_count,)), dma((x_count,)), dma((x_count,)),
            dma((z_count,)), dma((z_count,)), dma((stages,)), dma((stages,)),
        ],
        compiler_params=pltpu.CompilerParams(
            collective_id=0, has_side_effects=True, vmem_limit_bytes=VMEM_LIMIT
        ),
    )(
        tokens, norm_gain, q_weight, k_weight, v_weight, q_bias, k_bias, v_bias, positions,
        dest_slot, loss_mask, o_weight, jnp.asarray(table),
    )
    return pl.pallas_call(
        deliver,
        in_specs=[vmem, vmem],
        out_specs=[hbm, hbm],
        out_shape=[
            jax.ShapeDtypeStruct((part, out_width), BF16),
            jax.ShapeDtypeStruct((part,), F32),
        ],
        scratch_shapes=[pltpu.VMEM((part,), F32), dma((2,))],
    )(mixed, weight)


def solution(mesh):
    return jax.shard_map(
        per_device,
        mesh=mesh,
        in_specs=(
            P("dp", None),
            P(None, "dp"),
            P("dp"),
            P(),
            P("dp"),
            P(),
            P(None, "seq"),
            P(None, "seq"),
            P(None, "seq"),
            P("seq"),
            P("seq"),
            P("seq"),
            P("seq", None),
        ),
        out_specs=(P(("dp", "seq"), None), P(("dp", "seq"))),
        check_vma=False,
    )
```

```python
import functools
import math

import jax
import jax.numpy as jnp
import numpy as np
from jax import lax
from jax.experimental import pallas as pl
from jax.experimental.pallas import tpu as pltpu
from jax.sharding import PartitionSpec as P

DH = 128
BUCKET = 384
LANES = 128
PIECE = 256
QUADS, X_PAIRS, Z_PAIRS = 1, 2, 1
Y_AT, Z_AT = 0, 3
VMEM_LIMIT = 52000000

NORM_EPSILON = 1e-06
ROPE_BASE = 1000000.0
F32 = jnp.float32
BF16 = jnp.bfloat16


def iota(shape, axis):
    return lax.broadcasted_iota(jnp.int32, shape, axis)


HIGH, LOW = 64, 32
HIGH_ROWS, LOW_ROWS = 256, 128


def turn_tables():
    half_size = DH // 2
    pair = np.arange(half_size, dtype=np.float32)
    freq = np.exp(pair * np.float32(-2.0 * math.log(ROPE_BASE) / DH)).astype(np.float64)
    time_limit = DH // 8
    height_limit = time_limit + 3 * DH // 16
    axis_of = np.where(pair < time_limit, 0, np.where(pair < height_limit, 1, 2))
    sign = np.concatenate([-np.ones(half_size), np.ones(half_size)])
    blocks = []
    for count, step, rows in ((HIGH, LOW, HIGH_ROWS), (LOW, 1, LOW_ROWS)):
        table = np.zeros((rows, 2 * DH))
        for axis in range(3):
            angles = np.arange(count)[:, None] * float(step) * freq[None, :]
            chosen = (axis_of == axis)[None, :]
            cos = np.where(chosen, np.cos(angles), 0.0)
            sin = np.where(chosen, np.sin(angles), 0.0)
            at = slice(axis * count, (axis + 1) * count)
            table[at, :DH] = np.concatenate([cos, cos], axis=1)
            table[at, DH:] = np.concatenate([sin, sin], axis=1) * sign[None, :]
        top = table.astype(jnp.bfloat16)
        rest = (table - top.astype(np.float64)).astype(jnp.bfloat16)
        blocks += [top, rest]
    return np.concatenate(blocks, axis=0)


def rotary_tables(pos_ref, table, cos_out, sin_out):
    ids = pos_ref[...]
    rows = ids.shape[1]
    high = ids // LOW
    low = ids - high * LOW
    kind = iota((8, rows), 0)
    split = jnp.zeros((8, rows), jnp.int32)
    for axis in range(3):
        split = jnp.where(kind == 2 * axis, high[axis : axis + 1], split)
        split = jnp.where(kind == 2 * axis + 1, low[axis : axis + 1], split)
    width = HIGH_ROWS + LOW_ROWS
    column, row = iota((8, width), 1), iota((8, width), 0)
    low_at = column - HIGH_ROWS
    wanted = jnp.where(column < HIGH_ROWS, 2 * (column // HIGH), 2 * (low_at // LOW) + 1)
    spread = jnp.where(row == wanted, 1.0, 0.0).astype(BF16)
    told = lax.dot_general(
        split.astype(F32).astype(BF16), spread, (((0,), (0,)), ((), ())),
        preferred_element_type=F32,
    )
    at = iota((1, width), 1)
    value = jnp.where(
        at < HIGH_ROWS,
        jnp.where(at < 3 * HIGH, at % HIGH, -1),
        jnp.where(at < HIGH_ROWS + 3 * LOW, (at - HIGH_ROWS) % LOW, -1),
    ).astype(F32)
    hot = jnp.where(told == value, 1.0, 0.0).astype(BF16)
    hot_high, hot_low = hot[:, :HIGH_ROWS], hot[:, HIGH_ROWS:]
    low_from = 2 * HIGH_ROWS

    def look(one, first, count):
        return jnp.dot(one, table[first : first + count], preferred_element_type=F32) + jnp.dot(
            one, table[first + count : first + 2 * count], preferred_element_type=F32
        )

    big = look(hot_high, 0, HIGH_ROWS)
    small = look(hot_low, low_from, LOW_ROWS)
    cos_out[...] = big[:, :DH] * small[:, :DH] - big[:, DH:] * small[:, DH:]
    sin_out[...] = big[:, DH:] * small[:, :DH] + big[:, :DH] * small[:, DH:]


def pack_plan(peers, slot_count, group, room, slot_ref, mask_ref, select_out, info_out):
    rows = slot_ref.shape[0]
    slots = slot_ref[...][None, :]
    peer = slots // slot_count
    local = slots - peer * slot_count + 1
    mask = mask_ref[...][None, :].astype(F32)
    mask_sum = jnp.sum(mask, axis=1, keepdims=True)
    hot = jnp.where(iota((peers, rows), 0) == peer, 1.0, 0.0)
    earlier = jnp.where(iota((rows, rows), 0) < iota((rows, rows), 1), 1.0, 0.0).astype(BF16)
    counts = jnp.dot(hot.astype(BF16), earlier, preferred_element_type=F32)
    rank = jnp.sum(hot * counts, axis=0, keepdims=True).astype(jnp.int32)
    place = peer * room + rank
    high = local // 32
    kind = iota((8, rows), 0)
    facts = jnp.where(
        kind == 0,
        high.astype(F32),
        jnp.where(kind == 1, (local - high * 32).astype(F32), jnp.where(kind == 2, mask, 0.0)),
    ).astype(BF16)
    span = group * room
    spare = jnp.zeros((8, LANES - room), F32)
    for g in range(peers // group):
        select = jnp.where(iota((span, rows), 0) + g * span == place, 1.0, 0.0).astype(BF16)
        select_out[g * span : (g + 1) * span, :] = select
        told = lax.dot_general(facts, select, (((1,), (1,)), ((), ())), preferred_element_type=F32)
        told = jnp.where(iota(told.shape, 0) == 3, mask_sum, told)
        for p in range(group):
            one = told[:, p * room : (p + 1) * room]
            info_out[g * group + p] = jnp.concatenate([one, spare], axis=1)


def attend(q_slots, kv_slots, lengths, heads, per_kv, kv_count, ctx):
    start = 0
    scale = 1.0 / math.sqrt(DH)
    for size, length in zip((BUCKET, BUCKET // 2, BUCKET // 2), lengths):
        rows = slice(start, start + size)
        q_at, k_at = iota((size, size), 0), iota((size, size), 1)
        allowed = (q_at >= k_at) & (k_at < length)
        live = iota((size, DH), 0) < length
        for h in heads:
            pair = h // per_kv
            key = kv_slots[rows, pair * DH : (pair + 1) * DH]
            value = kv_slots[rows, (kv_count + pair) * DH : (kv_count + pair + 1) * DH]
            cols = slice(h * DH, (h + 1) * DH)
            scores = lax.dot_general(
                q_slots[rows, cols], key, (((1,), (1,)), ((), ())), preferred_element_type=F32
            )
            scores = jnp.where(allowed, scores * scale, -1e30)
            top = jnp.max(scores, axis=1, keepdims=True)
            weights = jnp.exp(scores - top)
            total = jnp.sum(weights, axis=1, keepdims=True)
            out = jnp.dot(weights.astype(BF16), value, preferred_element_type=F32) / total
            ctx[rows, cols] = jnp.where(live, out, 0.0).astype(BF16)
        start += size


def layer_kernel(
    peers, group, seq_count, q_heads, kv_heads, chunk, room, strips, pieces,
    tok_hbm, gain_hbm, qw_hbm, kw_hbm, vw_hbm, qb_hbm, kb_hbm, vb_hbm, pos_hbm,
    slot_hbm, mask_hbm, ow_hbm, table_hbm,
    mixed_ref, weight_ref,
    x, squares, qw, kvw, ow, table, pick, told_out, got_info, q_out, q_got, kv_out, kv_got,
    gain_ref, qb_ref, kb_ref, vb_ref, pos_ref, slot_ref, mask_ref,
    select, q_slots, kv_slots, ctx, ctx_far, w_far, held, pair, pair_in,
    far_pair, near_in, far_out, far_in, cos_ref, sin_ref, product,
    data_send, data_recv, info_send, info_recv, near_send, near_recv,
    pair_send, pair_recv, far_send, far_recv, load_sem,
    y_send, y_recv, x_send, x_recv, z_send, z_recv, ctx_send, ctx_recv, small_sem,
):
    me = lax.axis_index("dp")
    seat = lax.axis_index("seq")
    half = seat // 2
    core = seat % 2
    partner = half * 2 + (1 - core)
    across = (1 - half) * 2 + core
    a = me % 2
    b = (me // 2) % 2
    x_peer = me + 1 - 2 * a
    z_peer = me + 2 - 4 * b
    together = math.gcd(q_heads, 2)
    rows, depth = x.shape
    slot_count = q_slots.shape[0]
    part = slot_count // seq_count
    block_rows = 2 * part
    wide_cols = pieces * PIECE
    out_width = ow.shape[1]
    chunks = (out_width - wide_cols) // chunk
    strip = rows // strips
    kv_cols = kv_heads * DH

    barrier = pltpu.get_barrier_semaphore()
    for d in range(1, peers):
        pl.semaphore_signal(barrier, inc=1, device_id={"dp": (me + d) % peers})
    pl.semaphore_signal(barrier, inc=1, device_id={"seq": partner})
    pl.semaphore_signal(barrier, inc=1, device_id={"seq": across})
    token_loads = [
        pltpu.make_async_copy(
            tok_hbm.at[i * strip : (i + 1) * strip], x.at[i * strip : (i + 1) * strip],
            load_sem.at[i],
        )
        for i in range(strips)
    ]
    k_load = pltpu.make_async_copy(kw_hbm, kvw.at[:, :kv_cols], load_sem.at[strips])
    v_load = pltpu.make_async_copy(vw_hbm, kvw.at[:, kv_cols:], load_sem.at[strips + 1])
    q_load = pltpu.make_async_copy(qw_hbm, qw, load_sem.at[strips + 2])
    o_load = pltpu.make_async_copy(ow_hbm, ow, load_sem.at[strips + 3])
    table_load = pltpu.make_async_copy(table_hbm, table, load_sem.at[strips + 4])
    small_loads = [
        pltpu.make_async_copy(source, target, small_sem.at[i])
        for i, (source, target) in enumerate(
            (
                (slot_hbm, slot_ref), (mask_hbm, mask_ref), (pos_hbm, pos_ref),
                (gain_hbm, gain_ref), (kb_hbm, kb_ref), (vb_hbm, vb_ref), (qb_hbm, qb_ref),
            )
        )
    ]
    for copy in small_loads + [table_load] + token_loads + [k_load, v_load]:
        copy.start()

    y_own, x_jobs, z_jobs = [], [], []
    for k in range(QUADS):
        own = 4 * k + 2 * b + a
        y_at = len(y_own)
        y_own.append(own)
        z_at = len(z_jobs)
        z_jobs.append((own, y_at))
        x_jobs.append((own, "y", y_at))
        x_jobs.append((4 * k + 2 * (1 - b) + a, "z", z_at))
    for k in range(X_PAIRS):
        own = 4 * QUADS + 2 * k + a
        x_jobs.append((own, "y", len(y_own)))
        y_own.append(own)
    for k in range(Z_PAIRS):
        own = 4 * QUADS + 2 * X_PAIRS + 2 * k + b
        z_jobs.append((own, len(y_own)))
        y_own.append(own)

    def y_copy(i):
        at = pl.multiple_of(y_own[i] * PIECE, PIECE)
        return pltpu.make_async_remote_copy(
            ow_hbm.at[:, pl.ds(at, PIECE)], w_far.at[y_own[i]], y_send.at[i], y_recv.at[i],
            device_id={"seq": across},
        )

    def x_copy(i):
        own = x_jobs[i][0]
        return pltpu.make_async_remote_copy(
            w_far.at[own], w_far.at[own], x_send.at[i], x_recv.at[i], device_id={"dp": x_peer}
        )

    def z_copy(i):
        own = z_jobs[i][0]
        return pltpu.make_async_remote_copy(
            w_far.at[own], w_far.at[own], z_send.at[i], z_recv.at[i], device_id={"dp": z_peer}
        )

    def from_y(i):
        y_copy(i).wait_recv()
        for n, (_, source, at) in enumerate(x_jobs):
            if source == "y" and at == i:
                x_copy(n).start()
        for n, (_, at) in enumerate(z_jobs):
            if at == i:
                z_copy(n).start()

    def from_z(i):
        z_copy(i).wait_recv()
        for n, (_, source, at) in enumerate(x_jobs):
            if source == "z" and at == i:
                x_copy(n).start()

    small_loads[0].wait()
    small_loads[1].wait()
    pack_plan(peers, slot_count, group, room, slot_ref, mask_ref, pick, told_out)
    for copy in small_loads[2:]:
        copy.wait()
    table_load.wait()
    rotary_tables(pos_ref, table, cos_ref, sin_ref)
    gain = gain_ref[...][None, :]

    def info_copy(d):
        to = (me + d) % peers
        return pltpu.make_async_remote_copy(
            told_out.at[to], got_info.at[me], info_send.at[d], info_recv.at[d],
            device_id={"dp": to},
        )

    def ctx_copy(h):
        cols = slice(h * DH, (h + 1) * DH)
        return pltpu.make_async_remote_copy(
            ctx.at[pl.ds(pl.multiple_of((1 - half) * block_rows, block_rows), block_rows), cols],
            ctx_far.at[:, cols], ctx_send.at[h], ctx_recv.at[h],
            device_id={"seq": across},
        )

    def data_copy(stage, d):
        to = (me + d) % peers
        source, target = (kv_out, kv_got) if stage == 0 else (q_out, q_got)
        if stage > 0:
            source, target = source.at[stage - 1], target.at[stage - 1]
        return pltpu.make_async_remote_copy(
            source.at[to], target.at[me], data_send.at[stage, d], data_recv.at[stage, d],
            device_id={"dp": to},
        )

    def turn(wide):
        return wide * cos_ref[...] + pltpu.roll(wide, DH // 2, 1) * sin_ref[...]

    def pack(values, targets):
        span = group * room
        for g in range(peers // group):
            moved = jnp.dot(
                pick[g * span : (g + 1) * span, :], values, preferred_element_type=F32
            ).astype(BF16)
            first = 0
            for target in targets:
                width = target.shape[2]
                for p in range(group):
                    target[g * group + p] = moved[
                        p * room : (p + 1) * room, first : first + width
                    ]
                first += width

    def send(stage):
        for d in range(1, peers):
            data_copy(stage, d).start()
        source, kept = (kv_out, kv_got) if stage == 0 else (q_out, q_got)
        if stage > 0:
            source, kept = source.at[stage - 1], kept.at[stage - 1]
        kept[me] = source[me]

    def norm(i):
        at = slice(i * strip, (i + 1) * strip)
        total = jnp.zeros((strip, LANES), F32)
        for c in range(depth // LANES):
            cols = slice(c * LANES, (c + 1) * LANES)
            entry = x[at, cols].astype(F32)
            total = total + entry * entry
            x[at, cols] = (entry * gain[:, cols]).astype(BF16)
        squares[at, :] = jnp.sum(total, axis=1, keepdims=True)

    for i in range(strips // 2):
        token_loads[i].wait()
        norm(i)
    for i in range(strips // 2, strips):
        token_loads[i].wait()
    k_load.wait()
    v_load.wait()
    q_load.start()
    top = strips // 2 * strip
    for i in range(strips // 2, strips):
        norm(i)
    product[:top] = jnp.dot(x[:top], kvw[...], preferred_element_type=F32)
    product[top:] = jnp.dot(x[top:], kvw[...], preferred_element_type=F32)
    inverse = lax.rsqrt(squares[...] * (1.0 / depth) + NORM_EPSILON)
    heads_out = []
    for h in range(2 * kv_heads):
        bias_ref, at = (kb_ref, h) if h < kv_heads else (vb_ref, h - kv_heads)
        bias = bias_ref[at * DH : (at + 1) * DH][None, :]
        head = (product[:, h * DH : (h + 1) * DH] * inverse + bias).astype(BF16)
        if h < kv_heads:
            head = turn(head.astype(F32)).astype(BF16)
        heads_out.append(head)
    pack(jnp.concatenate(heads_out, axis=1), [kv_out])
    pl.semaphore_wait(barrier, peers + 1)
    send(0)
    for i in range(len(y_own)):
        y_copy(i).start()
    for d in range(1, peers):
        info_copy(d).start()
    got_info[me] = told_out[me]
    q_load.wait()
    o_load.start()
    for first in range(0, q_heads, together):
        cols = slice(first * DH, (first + together) * DH)
        made = jnp.dot(x[...], qw[:, cols], preferred_element_type=F32)
        heads_out = []
        for i in range(together):
            h = first + i
            bias = qb_ref[h * DH : (h + 1) * DH][None, :]
            head = (made[:, i * DH : (i + 1) * DH] * inverse + bias).astype(BF16)
            heads_out.append(turn(head.astype(F32)).astype(BF16))
        pack(
            jnp.concatenate(heads_out, axis=1), [q_out.at[first + i] for i in range(together)]
        )
        for i in range(together):
            send(first + i + 1)

    for d in range(1, peers):
        info_copy(d).wait()
    facts = jnp.concatenate([got_info[p][:, :room] for p in range(peers)], axis=1)
    count = jnp.zeros((1, 1), F32)
    for p in range(peers):
        count = count + got_info[p][3:4, :1]
    local = facts[0:1] * 32.0 + facts[1:2] - 1.0
    starts = (0, BUCKET, BUCKET + BUCKET // 2, 2 * BUCKET)
    lengths = []
    for bucket in range(3):
        inside = (local >= float(starts[bucket])) & (local < float(starts[bucket + 1]))
        filled = jnp.sum(jnp.where(inside, 1.0, 0.0), axis=1, keepdims=True)
        lengths.append(filled.astype(jnp.int32))
    slot_at = iota((slot_count, peers * room), 0).astype(F32)
    select[...] = jnp.where(slot_at == local, 1.0, 0.0).astype(BF16)
    own_select = select[pl.ds(pl.multiple_of(seat * part, part), part), :]
    seen = lax.dot_general(
        facts.astype(BF16), own_select, (((1,), (1,)), ((), ())), preferred_element_type=F32
    )
    weight_ref[...] = seen[2:3] * ((peers * rows) / count)

    def place(stage):
        for d in range(1, peers):
            data_copy(stage, d).wait()
        source = kv_got if stage == 0 else q_got.at[stage - 1]
        rows_got = source[...].reshape(peers * room, source.shape[2])
        return jnp.dot(select[...], rows_got, preferred_element_type=F32).astype(BF16)

    y_count, z_count = len(y_own), len(z_jobs)
    last = q_heads
    for stage in range(q_heads + 1):
        for i in range(y_count):
            if min(i + Y_AT, last) == stage:
                from_y(i)
        for i in range(QUADS):
            if min(Z_AT, last) == stage:
                from_z(i)
        if stage == 0:
            kv_slots[...] = place(0)
            continue
        h = stage - 1
        q_slots[:, h * DH : (h + 1) * DH] = place(stage)
        attend(q_slots, kv_slots, lengths, [h], q_heads // kv_heads, kv_heads, ctx)
        ctx_copy(h).start()
    o_load.wait()

    def near_copy(j):
        to_row = pl.multiple_of((1 - core) * part, part)
        cols = slice(j * chunk, (j + 1) * chunk)
        return pltpu.make_async_remote_copy(
            far_pair.at[pl.ds(to_row, part), cols], near_in.at[:, cols],
            near_send.at[j], near_recv.at[j], device_id={"seq": partner},
        )

    def far_copy(j):
        cols = slice(j * chunk, (j + 1) * chunk)
        return pltpu.make_async_remote_copy(
            far_out.at[:, cols], far_in.at[:, cols], far_send.at[j], far_recv.at[j],
            device_id={"seq": across},
        )

    groups = [(i * PIECE, PIECE) for i in range(pieces)]
    groups += [(wide_cols + j * chunk, chunk) for j in range(chunks)]

    def pair_copy(n):
        first, width = groups[n]
        to_row = pl.multiple_of((1 - core) * part, part)
        return pltpu.make_async_remote_copy(
            pair.at[pl.ds(to_row, part), first : first + width],
            pair_in.at[:, first : first + width],
            pair_send.at[n], pair_recv.at[n], device_id={"seq": partner},
        )

    mine_at = pl.multiple_of(half * block_rows, block_rows)
    far_at = pl.multiple_of((1 - half) * block_rows, block_rows)
    own_at = pl.multiple_of(core * part, part)

    def forward(j):
        near_copy(j).wait_recv()
        cols = slice(j * chunk, (j + 1) * chunk)
        kept = far_pair[pl.ds(own_at, part), cols].astype(F32)
        far_out[:, cols] = (kept + near_in[:, cols].astype(F32)).astype(BF16)
        far_copy(j).start()

    for j in range(chunks):
        cols = slice(j * chunk, (j + 1) * chunk)
        w = ow[:, wide_cols + j * chunk : wide_cols + (j + 1) * chunk]
        far_pair[:, cols] = jnp.dot(
            ctx[pl.ds(far_at, block_rows), :], w, preferred_element_type=F32
        ).astype(BF16)
        near_copy(j).start()
        if j > 0:
            forward(j - 1)
    if chunks:
        forward(chunks - 1)
    for j in range(chunks):
        first, width = groups[pieces + j]
        pair[:, first : first + width] = jnp.dot(
            ctx[pl.ds(mine_at, block_rows), :], ow[:, first : first + width],
            preferred_element_type=F32,
        ).astype(BF16)
        pair_copy(pieces + j).start()
    for i in range(pieces):
        held[:, i * PIECE : (i + 1) * PIECE] = jnp.dot(
            ctx[pl.ds(mine_at, block_rows), :], ow[:, i * PIECE : (i + 1) * PIECE],
            preferred_element_type=F32,
        )
    for h in range(q_heads):
        ctx_copy(h).wait()
    for i in range(y_count):
        y_copy(i).wait_send()

    def finish(which):
        for i in which:
            cols = slice(i * PIECE, (i + 1) * PIECE)
            pair[:, cols] = (
                held[:, cols] + jnp.dot(ctx_far[...], w_far[i], preferred_element_type=F32)
            ).astype(BF16)
        for i in which:
            pair_copy(i).start()

    x_first = 4 * QUADS
    z_first = x_first + 2 * X_PAIRS
    for k in range(X_PAIRS):
        x_copy(2 * QUADS + k).wait()
        finish(range(x_first + 2 * k, x_first + 2 * k + 2))
    for k in range(Z_PAIRS):
        z_copy(QUADS + k).wait()
        finish(range(z_first + 2 * k, z_first + 2 * k + 2))
    for k in range(QUADS):
        z_copy(k).wait_send()
        x_copy(2 * k).wait()
        x_copy(2 * k + 1).wait()
        finish(range(4 * k, 4 * k + 4))
    for n in list(range(pieces, pieces + chunks)) + list(range(pieces)):
        first, width = groups[n]
        cols = slice(first, first + width)
        pair_copy(n).wait()
        total = pair[pl.ds(own_at, part), cols].astype(F32) + pair_in[:, cols].astype(F32)
        if n >= pieces:
            j = n - pieces
            near_copy(j).wait_send()
            far_copy(j).wait()
            total = total + far_in[:, j * chunk : (j + 1) * chunk].astype(F32)
        mixed_ref[:, cols] = total.astype(BF16)


def deliver(mixed_in, weight_in, mixed_out, weight_out, flat, sems):
    big = pltpu.make_async_copy(mixed_in, mixed_out, sems.at[0])
    big.start()
    flat[...] = weight_in[0, :]
    small = pltpu.make_async_copy(flat, weight_out, sems.at[1])
    small.start()
    big.wait()
    small.wait()


def per_device(
    tokens, positions, loss_mask, sample_tokens, dest_slot, norm_gain,
    q_weight, k_weight, v_weight, q_bias, k_bias, v_bias, o_weight,
):
    peers = lax.axis_size("dp")
    seq_count = lax.axis_size("seq")
    rows, depth = tokens.shape
    slot_count = 2 * BUCKET
    room = -(-(slot_count // peers) // 16) * 16
    group = math.gcd(peers, 8)
    q_heads = q_weight.shape[1] // DH
    kv_heads = k_weight.shape[1] // DH
    strips = math.gcd(rows // 16, 4)
    part = slot_count // seq_count
    out_width = o_weight.shape[1]
    pieces = 4 * QUADS + 2 * X_PAIRS + 2 * Z_PAIRS
    wide_cols = pieces * PIECE
    narrow = out_width - wide_cols
    chunk = math.gcd(narrow, 512)
    chunks = narrow // chunk
    kv_width = 2 * kv_heads * DH
    y_count = QUADS + X_PAIRS + Z_PAIRS
    x_count = 2 * QUADS + X_PAIRS
    z_count = QUADS + Z_PAIRS
    vmem = pl.BlockSpec(memory_space=pltpu.VMEM)
    hbm = pl.BlockSpec(memory_space=pltpu.HBM)
    dma = pltpu.SemaphoreType.DMA
    table = turn_tables()
    buffers = [
        pltpu.VMEM((rows, depth), BF16),
        pltpu.VMEM((rows, 1), F32),
        pltpu.VMEM(q_weight.shape, BF16),
        pltpu.VMEM((depth, kv_width), BF16),
        pltpu.VMEM(o_weight.shape, BF16),
        pltpu.VMEM(table.shape, BF16),
        pltpu.VMEM((peers * room, rows), BF16),
        pltpu.VMEM((peers, 8, LANES), F32),
        pltpu.VMEM((peers, 8, LANES), F32),
        pltpu.VMEM((q_heads, peers, room, DH), BF16),
        pltpu.VMEM((q_heads, peers, room, DH), BF16),
        pltpu.VMEM((peers, room, kv_width), BF16),
        pltpu.VMEM((peers, room, kv_width), BF16),
        pltpu.VMEM(norm_gain.shape, F32),
        pltpu.VMEM(q_bias.shape, F32),
        pltpu.VMEM(k_bias.shape, F32),
        pltpu.VMEM(v_bias.shape, F32),
        pltpu.VMEM(positions.shape, jnp.int32),
        pltpu.VMEM(dest_slot.shape, jnp.int32),
        pltpu.VMEM(loss_mask.shape, jnp.int32),
        pltpu.VMEM((slot_count, peers * room), BF16),
        pltpu.VMEM((slot_count, q_heads * DH), BF16),
        pltpu.VMEM((slot_count, kv_width), BF16),
        pltpu.VMEM((slot_count, q_heads * DH), BF16),
        pltpu.VMEM((2 * part, q_heads * DH), BF16),
        pltpu.VMEM((pieces, o_weight.shape[0], PIECE), BF16),
        pltpu.VMEM((2 * part, wide_cols), F32),
        pltpu.VMEM((2 * part, out_width), BF16),
        pltpu.VMEM((part, out_width), BF16),
        pltpu.VMEM((2 * part, narrow), BF16),
        pltpu.VMEM((part, narrow), BF16),
        pltpu.VMEM((part, narrow), BF16),
        pltpu.VMEM((part, narrow), BF16),
        pltpu.VMEM((rows, DH), F32),
        pltpu.VMEM((rows, DH), F32),
        pltpu.VMEM((rows, kv_width), F32),
    ]
    operands = (
        tokens, norm_gain, q_weight, k_weight, v_weight, q_bias, k_bias, v_bias, positions,
        dest_slot, loss_mask, o_weight, jnp.asarray(table),
    )
    mixed, weight = pl.pallas_call(
        functools.partial(
            layer_kernel, peers, group, seq_count, q_heads, kv_heads, chunk, room, strips, pieces
        ),
        in_specs=[
            hbm, hbm, hbm, hbm, hbm, hbm, hbm, hbm, hbm, hbm, hbm, hbm, hbm,
        ],
        out_specs=[vmem, vmem],
        out_shape=[
            jax.ShapeDtypeStruct((part, out_width), BF16),
            jax.ShapeDtypeStruct((1, part), F32),
        ],
        scratch_shapes=buffers + [
            dma((q_heads + 1, peers)), dma((q_heads + 1, peers)), dma((peers,)), dma((peers,)),
            dma((chunks,)), dma((chunks,)), dma((pieces + chunks,)), dma((pieces + chunks,)),
            dma((chunks,)), dma((chunks,)), dma((strips + 5,)),
            dma((y_count,)), dma((y_count,)), dma((x_count,)), dma((x_count,)),
            dma((z_count,)), dma((z_count,)), dma((q_heads,)), dma((q_heads,)), dma((7,)),
        ],
        compiler_params=pltpu.CompilerParams(
            collective_id=0, has_side_effects=True, vmem_limit_bytes=VMEM_LIMIT
        ),
    )(*(pltpu.with_memory_space_constraint(one, pltpu.HBM) for one in operands))
    return pl.pallas_call(
        deliver,
        in_specs=[vmem, vmem],
        out_specs=[hbm, hbm],
        out_shape=[
            jax.ShapeDtypeStruct((part, out_width), BF16),
            jax.ShapeDtypeStruct((part,), F32),
        ],
        scratch_shapes=[pltpu.VMEM((part,), F32), dma((2,))],
        compiler_params=pltpu.CompilerParams(vmem_limit_bytes=4 * 2**20),
    )(mixed, weight)


def solution(mesh):
    return jax.shard_map(
        per_device,
        mesh=mesh,
        in_specs=(
            P("dp", None),
            P(None, "dp"),
            P("dp"),
            P(),
            P("dp"),
            P(),
            P(None, "seq"),
            P(None, "seq"),
            P(None, "seq"),
            P("seq"),
            P("seq"),
            P("seq"),
            P("seq", None),
        ),
        out_specs=(P(("dp", "seq"), None), P(("dp", "seq"))),
        check_vma=False,
    )
```

```python
import functools
import math

import jax
import jax.numpy as jnp
import numpy as np
from jax import lax
from jax.experimental import pallas as pl
from jax.experimental.pallas import tpu as pltpu
from jax.sharding import PartitionSpec as P

DH = 128
BUCKET = 384
LANES = 128
PIECE = 256
QUADS, X_PAIRS, Z_PAIRS = 1, 2, 2
Y_AT, Z_AT = 0, 4
VMEM_LIMIT = 52000000

NORM_EPSILON = 1e-06
ROPE_BASE = 1000000.0
F32 = jnp.float32
BF16 = jnp.bfloat16


def iota(shape, axis):
    return lax.broadcasted_iota(jnp.int32, shape, axis)


HIGH, LOW = 64, 32
HIGH_ROWS, LOW_ROWS = 256, 128


def turn_tables():
    half_size = DH // 2
    pair = np.arange(half_size, dtype=np.float32)
    freq = np.exp(pair * np.float32(-2.0 * math.log(ROPE_BASE) / DH)).astype(np.float64)
    time_limit = DH // 8
    height_limit = time_limit + 3 * DH // 16
    axis_of = np.where(pair < time_limit, 0, np.where(pair < height_limit, 1, 2))
    sign = np.concatenate([-np.ones(half_size), np.ones(half_size)])
    blocks = []
    for count, step, rows in ((HIGH, LOW, HIGH_ROWS), (LOW, 1, LOW_ROWS)):
        table = np.zeros((rows, 2 * DH))
        for axis in range(3):
            angles = np.arange(count)[:, None] * float(step) * freq[None, :]
            chosen = (axis_of == axis)[None, :]
            cos = np.where(chosen, np.cos(angles), 0.0)
            sin = np.where(chosen, np.sin(angles), 0.0)
            at = slice(axis * count, (axis + 1) * count)
            table[at, :DH] = np.concatenate([cos, cos], axis=1)
            table[at, DH:] = np.concatenate([sin, sin], axis=1) * sign[None, :]
        top = table.astype(jnp.bfloat16)
        rest = (table - top.astype(np.float64)).astype(jnp.bfloat16)
        blocks += [top, rest]
    return np.concatenate(blocks, axis=0)


def rotary_tables(pos_ref, table, cos_out, sin_out):
    ids = pos_ref[...]
    rows = ids.shape[1]
    high = ids // LOW
    low = ids - high * LOW
    kind = iota((8, rows), 0)
    split = jnp.zeros((8, rows), jnp.int32)
    for axis in range(3):
        split = jnp.where(kind == 2 * axis, high[axis : axis + 1], split)
        split = jnp.where(kind == 2 * axis + 1, low[axis : axis + 1], split)
    width = HIGH_ROWS + LOW_ROWS
    column, row = iota((8, width), 1), iota((8, width), 0)
    low_at = column - HIGH_ROWS
    wanted = jnp.where(column < HIGH_ROWS, 2 * (column // HIGH), 2 * (low_at // LOW) + 1)
    spread = jnp.where(row == wanted, 1.0, 0.0).astype(BF16)
    told = lax.dot_general(
        split.astype(F32).astype(BF16), spread, (((0,), (0,)), ((), ())),
        preferred_element_type=F32,
    )
    at = iota((1, width), 1)
    value = jnp.where(
        at < HIGH_ROWS,
        jnp.where(at < 3 * HIGH, at % HIGH, -1),
        jnp.where(at < HIGH_ROWS + 3 * LOW, (at - HIGH_ROWS) % LOW, -1),
    ).astype(F32)
    hot = jnp.where(told == value, 1.0, 0.0).astype(BF16)
    hot_high, hot_low = hot[:, :HIGH_ROWS], hot[:, HIGH_ROWS:]
    low_from = 2 * HIGH_ROWS

    def look(one, first, count):
        return jnp.dot(one, table[first : first + count], preferred_element_type=F32) + jnp.dot(
            one, table[first + count : first + 2 * count], preferred_element_type=F32
        )

    big = look(hot_high, 0, HIGH_ROWS)
    small = look(hot_low, low_from, LOW_ROWS)
    cos_out[...] = big[:, :DH] * small[:, :DH] - big[:, DH:] * small[:, DH:]
    sin_out[...] = big[:, DH:] * small[:, :DH] + big[:, :DH] * small[:, DH:]


def pack_plan(peers, slot_count, group, room, slot_ref, mask_ref, select_out, info_out):
    rows = slot_ref.shape[0]
    slots = slot_ref[...][None, :]
    peer = slots // slot_count
    local = slots - peer * slot_count + 1
    mask = mask_ref[...][None, :].astype(F32)
    mask_sum = jnp.sum(mask, axis=1, keepdims=True)
    hot = jnp.where(iota((peers, rows), 0) == peer, 1.0, 0.0)
    earlier = jnp.where(iota((rows, rows), 0) < iota((rows, rows), 1), 1.0, 0.0).astype(BF16)
    counts = jnp.dot(hot.astype(BF16), earlier, preferred_element_type=F32)
    rank = jnp.sum(hot * counts, axis=0, keepdims=True).astype(jnp.int32)
    place = peer * room + rank
    high = local // 32
    kind = iota((8, rows), 0)
    facts = jnp.where(
        kind == 0,
        high.astype(F32),
        jnp.where(kind == 1, (local - high * 32).astype(F32), jnp.where(kind == 2, mask, 0.0)),
    ).astype(BF16)
    span = group * room
    spare = jnp.zeros((8, LANES - room), F32)
    for g in range(peers // group):
        select = jnp.where(iota((span, rows), 0) + g * span == place, 1.0, 0.0).astype(BF16)
        select_out[g * span : (g + 1) * span, :] = select
        told = lax.dot_general(facts, select, (((1,), (1,)), ((), ())), preferred_element_type=F32)
        told = jnp.where(iota(told.shape, 0) == 3, mask_sum, told)
        for p in range(group):
            one = told[:, p * room : (p + 1) * room]
            info_out[g * group + p] = jnp.concatenate([one, spare], axis=1)


def attend(q_slots, kv_slots, lengths, heads, per_kv, kv_count, ctx):
    start = 0
    scale = 1.0 / math.sqrt(DH)
    for size, length in zip((BUCKET, BUCKET // 2, BUCKET // 2), lengths):
        rows = slice(start, start + size)
        q_at, k_at = iota((size, size), 0), iota((size, size), 1)
        allowed = (q_at >= k_at) & (k_at < length)
        live = iota((size, DH), 0) < length
        for h in heads:
            pair = h // per_kv
            key = kv_slots[rows, pair * DH : (pair + 1) * DH]
            value = kv_slots[rows, (kv_count + pair) * DH : (kv_count + pair + 1) * DH]
            cols = slice(h * DH, (h + 1) * DH)
            scores = lax.dot_general(
                q_slots[rows, cols], key, (((1,), (1,)), ((), ())), preferred_element_type=F32
            )
            scores = jnp.where(allowed, scores * scale, -1e30)
            top = jnp.max(scores, axis=1, keepdims=True)
            weights = jnp.exp(scores - top)
            total = jnp.sum(weights, axis=1, keepdims=True)
            out = jnp.dot(weights.astype(BF16), value, preferred_element_type=F32) / total
            ctx[rows, cols] = jnp.where(live, out, 0.0).astype(BF16)
        start += size


def layer_kernel(
    peers, group, seq_count, q_heads, kv_heads, chunk, room, strips, pieces,
    tok_hbm, gain_hbm, qw_hbm, kw_hbm, vw_hbm, qb_hbm, kb_hbm, vb_hbm, pos_hbm,
    slot_hbm, mask_hbm, ow_hbm, table_hbm,
    mixed_ref, weight_ref,
    x, squares, qw, kvw, ow, table, pick, told_out, got_info, q_out, q_got, kv_out, kv_got,
    gain_ref, qb_ref, kb_ref, vb_ref, pos_ref, slot_ref, mask_ref,
    select, q_slots, kv_slots, ctx, ctx_far, w_far, held, pair, pair_in,
    far_pair, near_in, far_out, far_in, cos_ref, sin_ref, product,
    data_send, data_recv, info_send, info_recv, near_send, near_recv,
    pair_send, pair_recv, far_send, far_recv, load_sem,
    y_send, y_recv, x_send, x_recv, z_send, z_recv, ctx_send, ctx_recv, small_sem,
):
    me = lax.axis_index("dp")
    seat = lax.axis_index("seq")
    half = seat // 2
    core = seat % 2
    partner = half * 2 + (1 - core)
    across = (1 - half) * 2 + core
    a = me % 2
    b = (me // 2) % 2
    x_peer = me + 1 - 2 * a
    z_peer = me + 2 - 4 * b
    together = math.gcd(q_heads, 2)
    rows, depth = x.shape
    slot_count = q_slots.shape[0]
    part = slot_count // seq_count
    block_rows = 2 * part
    wide_cols = pieces * PIECE
    out_width = ow.shape[1]
    chunks = (out_width - wide_cols) // chunk
    strip = rows // strips
    kv_cols = kv_heads * DH

    barrier = pltpu.get_barrier_semaphore()
    for d in range(1, peers):
        pl.semaphore_signal(barrier, inc=1, device_id={"dp": (me + d) % peers})
    pl.semaphore_signal(barrier, inc=1, device_id={"seq": partner})
    pl.semaphore_signal(barrier, inc=1, device_id={"seq": across})
    token_loads = [
        pltpu.make_async_copy(
            tok_hbm.at[i * strip : (i + 1) * strip], x.at[i * strip : (i + 1) * strip],
            load_sem.at[i],
        )
        for i in range(strips)
    ]
    k_load = pltpu.make_async_copy(kw_hbm, kvw.at[:, :kv_cols], load_sem.at[strips])
    v_load = pltpu.make_async_copy(vw_hbm, kvw.at[:, kv_cols:], load_sem.at[strips + 1])
    q_load = pltpu.make_async_copy(qw_hbm, qw, load_sem.at[strips + 2])
    o_load = pltpu.make_async_copy(ow_hbm, ow, load_sem.at[strips + 3])
    table_load = pltpu.make_async_copy(table_hbm, table, load_sem.at[strips + 4])
    small_loads = [
        pltpu.make_async_copy(source, target, small_sem.at[i])
        for i, (source, target) in enumerate(
            (
                (slot_hbm, slot_ref), (mask_hbm, mask_ref), (pos_hbm, pos_ref),
                (gain_hbm, gain_ref), (kb_hbm, kb_ref), (vb_hbm, vb_ref), (qb_hbm, qb_ref),
            )
        )
    ]
    for copy in small_loads + [table_load] + token_loads + [k_load, v_load]:
        copy.start()

    y_own, x_jobs, z_jobs = [], [], []
    for k in range(QUADS):
        own = 4 * k + 2 * b + a
        y_at = len(y_own)
        y_own.append(own)
        z_at = len(z_jobs)
        z_jobs.append((own, y_at))
        x_jobs.append((own, "y", y_at))
        x_jobs.append((4 * k + 2 * (1 - b) + a, "z", z_at))
    for k in range(X_PAIRS):
        own = 4 * QUADS + 2 * k + a
        x_jobs.append((own, "y", len(y_own)))
        y_own.append(own)
    for k in range(Z_PAIRS):
        own = 4 * QUADS + 2 * X_PAIRS + 2 * k + b
        z_jobs.append((own, len(y_own)))
        y_own.append(own)

    def y_copy(i):
        at = pl.multiple_of(y_own[i] * PIECE, PIECE)
        return pltpu.make_async_remote_copy(
            ow_hbm.at[:, pl.ds(at, PIECE)], w_far.at[y_own[i]], y_send.at[i], y_recv.at[i],
            device_id={"seq": across},
        )

    def x_copy(i):
        own = x_jobs[i][0]
        return pltpu.make_async_remote_copy(
            w_far.at[own], w_far.at[own], x_send.at[i], x_recv.at[i], device_id={"dp": x_peer}
        )

    def z_copy(i):
        own = z_jobs[i][0]
        return pltpu.make_async_remote_copy(
            w_far.at[own], w_far.at[own], z_send.at[i], z_recv.at[i], device_id={"dp": z_peer}
        )

    def from_y(i):
        y_copy(i).wait_recv()
        for n, (_, source, at) in enumerate(x_jobs):
            if source == "y" and at == i:
                x_copy(n).start()
        for n, (_, at) in enumerate(z_jobs):
            if at == i:
                z_copy(n).start()

    def from_z(i):
        z_copy(i).wait_recv()
        for n, (_, source, at) in enumerate(x_jobs):
            if source == "z" and at == i:
                x_copy(n).start()

    small_loads[0].wait()
    small_loads[1].wait()
    pack_plan(peers, slot_count, group, room, slot_ref, mask_ref, pick, told_out)
    for copy in small_loads[2:]:
        copy.wait()
    table_load.wait()
    rotary_tables(pos_ref, table, cos_ref, sin_ref)
    gain = gain_ref[...][None, :]

    def info_copy(d):
        to = (me + d) % peers
        return pltpu.make_async_remote_copy(
            told_out.at[to], got_info.at[me], info_send.at[d], info_recv.at[d],
            device_id={"dp": to},
        )

    def ctx_copy(h):
        cols = slice(h * DH, (h + 1) * DH)
        return pltpu.make_async_remote_copy(
            ctx.at[pl.ds(pl.multiple_of((1 - half) * block_rows, block_rows), block_rows), cols],
            ctx_far.at[:, cols], ctx_send.at[h], ctx_recv.at[h],
            device_id={"seq": across},
        )

    def data_copy(stage, d):
        to = (me + d) % peers
        source, target = (kv_out, kv_got) if stage == 0 else (q_out, q_got)
        if stage > 0:
            source, target = source.at[stage - 1], target.at[stage - 1]
        return pltpu.make_async_remote_copy(
            source.at[to], target.at[me], data_send.at[stage, d], data_recv.at[stage, d],
            device_id={"dp": to},
        )

    def turn(wide):
        return wide * cos_ref[...] + pltpu.roll(wide, DH // 2, 1) * sin_ref[...]

    def pack(values, targets):
        span = group * room
        for g in range(peers // group):
            moved = jnp.dot(
                pick[g * span : (g + 1) * span, :], values, preferred_element_type=F32
            ).astype(BF16)
            first = 0
            for target in targets:
                width = target.shape[2]
                for p in range(group):
                    target[g * group + p] = moved[
                        p * room : (p + 1) * room, first : first + width
                    ]
                first += width

    def send(stage):
        for d in range(1, peers):
            data_copy(stage, d).start()
        source, kept = (kv_out, kv_got) if stage == 0 else (q_out, q_got)
        if stage > 0:
            source, kept = source.at[stage - 1], kept.at[stage - 1]
        kept[me] = source[me]

    def norm(i):
        at = slice(i * strip, (i + 1) * strip)
        total = jnp.zeros((strip, LANES), F32)
        for c in range(depth // LANES):
            cols = slice(c * LANES, (c + 1) * LANES)
            entry = x[at, cols].astype(F32)
            total = total + entry * entry
            x[at, cols] = (entry * gain[:, cols]).astype(BF16)
        squares[at, :] = jnp.sum(total, axis=1, keepdims=True)

    for i in range(strips // 2):
        token_loads[i].wait()
        norm(i)
    pl.semaphore_wait(barrier, peers + 1)
    for i in range(len(y_own)):
        y_copy(i).start()
    for d in range(1, peers):
        info_copy(d).start()
    got_info[me] = told_out[me]
    for i in range(strips // 2, strips):
        token_loads[i].wait()
    k_load.wait()
    v_load.wait()
    q_load.start()
    top = strips // 2 * strip
    for i in range(strips // 2, strips):
        norm(i)
    product[:top] = jnp.dot(x[:top], kvw[...], preferred_element_type=F32)
    product[top:] = jnp.dot(x[top:], kvw[...], preferred_element_type=F32)
    inverse = lax.rsqrt(squares[...] * (1.0 / depth) + NORM_EPSILON)
    heads_out = []
    for h in range(2 * kv_heads):
        bias_ref, at = (kb_ref, h) if h < kv_heads else (vb_ref, h - kv_heads)
        bias = bias_ref[at * DH : (at + 1) * DH][None, :]
        head = (product[:, h * DH : (h + 1) * DH] * inverse + bias).astype(BF16)
        if h < kv_heads:
            head = turn(head.astype(F32)).astype(BF16)
        heads_out.append(head)
    pack(jnp.concatenate(heads_out, axis=1), [kv_out])
    send(0)
    q_load.wait()
    o_load.start()
    for first in range(0, q_heads, together):
        cols = slice(first * DH, (first + together) * DH)
        made = jnp.dot(x[...], qw[:, cols], preferred_element_type=F32)
        heads_out = []
        for i in range(together):
            h = first + i
            bias = qb_ref[h * DH : (h + 1) * DH][None, :]
            head = (made[:, i * DH : (i + 1) * DH] * inverse + bias).astype(BF16)
            heads_out.append(turn(head.astype(F32)).astype(BF16))
        pack(
            jnp.concatenate(heads_out, axis=1), [q_out.at[first + i] for i in range(together)]
        )
        for i in range(together):
            send(first + i + 1)

    for d in range(1, peers):
        info_copy(d).wait()
    facts = jnp.concatenate([got_info[p][:, :room] for p in range(peers)], axis=1)
    count = jnp.zeros((1, 1), F32)
    for p in range(peers):
        count = count + got_info[p][3:4, :1]
    local = facts[0:1] * 32.0 + facts[1:2] - 1.0
    starts = (0, BUCKET, BUCKET + BUCKET // 2, 2 * BUCKET)
    lengths = []
    for bucket in range(3):
        inside = (local >= float(starts[bucket])) & (local < float(starts[bucket + 1]))
        filled = jnp.sum(jnp.where(inside, 1.0, 0.0), axis=1, keepdims=True)
        lengths.append(filled.astype(jnp.int32))
    slot_at = iota((slot_count, peers * room), 0).astype(F32)
    select[...] = jnp.where(slot_at == local, 1.0, 0.0).astype(BF16)
    own_select = select[pl.ds(pl.multiple_of(seat * part, part), part), :]
    seen = lax.dot_general(
        facts.astype(BF16), own_select, (((1,), (1,)), ((), ())), preferred_element_type=F32
    )
    weight_ref[...] = seen[2:3] * ((peers * rows) / count)

    def place(stage):
        for d in range(1, peers):
            data_copy(stage, d).wait()
        source = kv_got if stage == 0 else q_got.at[stage - 1]
        rows_got = source[...].reshape(peers * room, source.shape[2])
        return jnp.dot(select[...], rows_got, preferred_element_type=F32).astype(BF16)

    y_count, z_count = len(y_own), len(z_jobs)
    last = q_heads
    for stage in range(q_heads + 1):
        for i in range(y_count):
            if min(i + Y_AT, last) == stage:
                from_y(i)
        for i in range(QUADS):
            if min(Z_AT, last) == stage:
                from_z(i)
        if stage == 0:
            kv_slots[...] = place(0)
            continue
        h = stage - 1
        q_slots[:, h * DH : (h + 1) * DH] = place(stage)
        attend(q_slots, kv_slots, lengths, [h], q_heads // kv_heads, kv_heads, ctx)
        ctx_copy(h).start()
    o_load.wait()

    def near_copy(j):
        to_row = pl.multiple_of((1 - core) * part, part)
        cols = slice(j * chunk, (j + 1) * chunk)
        return pltpu.make_async_remote_copy(
            far_pair.at[pl.ds(to_row, part), cols], near_in.at[:, cols],
            near_send.at[j], near_recv.at[j], device_id={"seq": partner},
        )

    def far_copy(j):
        cols = slice(j * chunk, (j + 1) * chunk)
        return pltpu.make_async_remote_copy(
            far_out.at[:, cols], far_in.at[:, cols], far_send.at[j], far_recv.at[j],
            device_id={"seq": across},
        )

    groups = [(i * PIECE, PIECE) for i in range(pieces)]
    groups += [(wide_cols + j * chunk, chunk) for j in range(chunks)]

    def pair_copy(n):
        first, width = groups[n]
        to_row = pl.multiple_of((1 - core) * part, part)
        return pltpu.make_async_remote_copy(
            pair.at[pl.ds(to_row, part), first : first + width],
            pair_in.at[:, first : first + width],
            pair_send.at[n], pair_recv.at[n], device_id={"seq": partner},
        )

    mine_at = pl.multiple_of(half * block_rows, block_rows)
    far_at = pl.multiple_of((1 - half) * block_rows, block_rows)
    own_at = pl.multiple_of(core * part, part)

    def forward(j):
        near_copy(j).wait_recv()
        cols = slice(j * chunk, (j + 1) * chunk)
        kept = far_pair[pl.ds(own_at, part), cols].astype(F32)
        far_out[:, cols] = (kept + near_in[:, cols].astype(F32)).astype(BF16)
        far_copy(j).start()

    for j in range(chunks):
        cols = slice(j * chunk, (j + 1) * chunk)
        w = ow[:, wide_cols + j * chunk : wide_cols + (j + 1) * chunk]
        far_pair[:, cols] = jnp.dot(
            ctx[pl.ds(far_at, block_rows), :], w, preferred_element_type=F32
        ).astype(BF16)
        near_copy(j).start()
        if j > 0:
            forward(j - 1)
    if chunks:
        forward(chunks - 1)
    for j in range(chunks):
        first, width = groups[pieces + j]
        pair[:, first : first + width] = jnp.dot(
            ctx[pl.ds(mine_at, block_rows), :], ow[:, first : first + width],
            preferred_element_type=F32,
        ).astype(BF16)
        pair_copy(pieces + j).start()
    for i in range(pieces):
        held[:, i * PIECE : (i + 1) * PIECE] = jnp.dot(
            ctx[pl.ds(mine_at, block_rows), :], ow[:, i * PIECE : (i + 1) * PIECE],
            preferred_element_type=F32,
        )
    for h in range(q_heads):
        ctx_copy(h).wait()
    for i in range(y_count):
        y_copy(i).wait_send()

    def finish(which):
        for i in which:
            cols = slice(i * PIECE, (i + 1) * PIECE)
            pair[:, cols] = (
                held[:, cols] + jnp.dot(ctx_far[...], w_far[i], preferred_element_type=F32)
            ).astype(BF16)
        for i in which:
            pair_copy(i).start()

    x_first = 4 * QUADS
    z_first = x_first + 2 * X_PAIRS
    for k in range(X_PAIRS):
        x_copy(2 * QUADS + k).wait()
        finish(range(x_first + 2 * k, x_first + 2 * k + 2))
    for k in range(Z_PAIRS):
        z_copy(QUADS + k).wait()
        finish(range(z_first + 2 * k, z_first + 2 * k + 2))
    for k in range(QUADS):
        z_copy(k).wait_send()
        x_copy(2 * k).wait()
        x_copy(2 * k + 1).wait()
        finish(range(4 * k, 4 * k + 4))
    for n in list(range(pieces, pieces + chunks)) + list(range(pieces)):
        first, width = groups[n]
        cols = slice(first, first + width)
        pair_copy(n).wait()
        total = pair[pl.ds(own_at, part), cols].astype(F32) + pair_in[:, cols].astype(F32)
        if n >= pieces:
            j = n - pieces
            near_copy(j).wait_send()
            far_copy(j).wait()
            total = total + far_in[:, j * chunk : (j + 1) * chunk].astype(F32)
        mixed_ref[:, cols] = total.astype(BF16)


def deliver(mixed_in, weight_in, mixed_out, weight_out, flat, sems):
    big = pltpu.make_async_copy(mixed_in, mixed_out, sems.at[0])
    big.start()
    flat[...] = weight_in[0, :]
    small = pltpu.make_async_copy(flat, weight_out, sems.at[1])
    small.start()
    big.wait()
    small.wait()


def per_device(
    tokens, positions, loss_mask, sample_tokens, dest_slot, norm_gain,
    q_weight, k_weight, v_weight, q_bias, k_bias, v_bias, o_weight,
):
    peers = lax.axis_size("dp")
    seq_count = lax.axis_size("seq")
    rows, depth = tokens.shape
    slot_count = 2 * BUCKET
    room = -(-(slot_count // peers) // 16) * 16
    group = math.gcd(peers, 8)
    q_heads = q_weight.shape[1] // DH
    kv_heads = k_weight.shape[1] // DH
    strips = math.gcd(rows // 16, 4)
    part = slot_count // seq_count
    out_width = o_weight.shape[1]
    pieces = 4 * QUADS + 2 * X_PAIRS + 2 * Z_PAIRS
    wide_cols = pieces * PIECE
    narrow = out_width - wide_cols
    chunk = math.gcd(narrow, 512)
    chunks = narrow // chunk
    kv_width = 2 * kv_heads * DH
    y_count = QUADS + X_PAIRS + Z_PAIRS
    x_count = 2 * QUADS + X_PAIRS
    z_count = QUADS + Z_PAIRS
    vmem = pl.BlockSpec(memory_space=pltpu.VMEM)
    hbm = pl.BlockSpec(memory_space=pltpu.HBM)
    dma = pltpu.SemaphoreType.DMA
    table = turn_tables()
    buffers = [
        pltpu.VMEM((rows, depth), BF16),
        pltpu.VMEM((rows, 1), F32),
        pltpu.VMEM(q_weight.shape, BF16),
        pltpu.VMEM((depth, kv_width), BF16),
        pltpu.VMEM(o_weight.shape, BF16),
        pltpu.VMEM(table.shape, BF16),
        pltpu.VMEM((peers * room, rows), BF16),
        pltpu.VMEM((peers, 8, LANES), F32),
        pltpu.VMEM((peers, 8, LANES), F32),
        pltpu.VMEM((q_heads, peers, room, DH), BF16),
        pltpu.VMEM((q_heads, peers, room, DH), BF16),
        pltpu.VMEM((peers, room, kv_width), BF16),
        pltpu.VMEM((peers, room, kv_width), BF16),
        pltpu.VMEM(norm_gain.shape, F32),
        pltpu.VMEM(q_bias.shape, F32),
        pltpu.VMEM(k_bias.shape, F32),
        pltpu.VMEM(v_bias.shape, F32),
        pltpu.VMEM(positions.shape, jnp.int32),
        pltpu.VMEM(dest_slot.shape, jnp.int32),
        pltpu.VMEM(loss_mask.shape, jnp.int32),
        pltpu.VMEM((slot_count, peers * room), BF16),
        pltpu.VMEM((slot_count, q_heads * DH), BF16),
        pltpu.VMEM((slot_count, kv_width), BF16),
        pltpu.VMEM((slot_count, q_heads * DH), BF16),
        pltpu.VMEM((2 * part, q_heads * DH), BF16),
        pltpu.VMEM((pieces, o_weight.shape[0], PIECE), BF16),
        pltpu.VMEM((2 * part, wide_cols), F32),
        pltpu.VMEM((2 * part, out_width), BF16),
        pltpu.VMEM((part, out_width), BF16),
        pltpu.VMEM((2 * part, narrow), BF16),
        pltpu.VMEM((part, narrow), BF16),
        pltpu.VMEM((part, narrow), BF16),
        pltpu.VMEM((part, narrow), BF16),
        pltpu.VMEM((rows, DH), F32),
        pltpu.VMEM((rows, DH), F32),
        pltpu.VMEM((rows, kv_width), F32),
    ]
    operands = (
        tokens, norm_gain, q_weight, k_weight, v_weight, q_bias, k_bias, v_bias, positions,
        dest_slot, loss_mask, o_weight, jnp.asarray(table),
    )
    mixed, weight = pl.pallas_call(
        functools.partial(
            layer_kernel, peers, group, seq_count, q_heads, kv_heads, chunk, room, strips, pieces
        ),
        in_specs=[
            hbm, hbm, hbm, hbm, hbm, hbm, hbm, hbm, hbm, hbm, hbm, hbm, hbm,
        ],
        out_specs=[vmem, vmem],
        out_shape=[
            jax.ShapeDtypeStruct((part, out_width), BF16),
            jax.ShapeDtypeStruct((1, part), F32),
        ],
        scratch_shapes=buffers + [
            dma((q_heads + 1, peers)), dma((q_heads + 1, peers)), dma((peers,)), dma((peers,)),
            dma((chunks,)), dma((chunks,)), dma((pieces + chunks,)), dma((pieces + chunks,)),
            dma((chunks,)), dma((chunks,)), dma((strips + 5,)),
            dma((y_count,)), dma((y_count,)), dma((x_count,)), dma((x_count,)),
            dma((z_count,)), dma((z_count,)), dma((q_heads,)), dma((q_heads,)), dma((7,)),
        ],
        compiler_params=pltpu.CompilerParams(
            collective_id=0, has_side_effects=True, vmem_limit_bytes=VMEM_LIMIT
        ),
    )(*(pltpu.with_memory_space_constraint(one, pltpu.HBM) for one in operands))
    return pl.pallas_call(
        deliver,
        in_specs=[vmem, vmem],
        out_specs=[hbm, hbm],
        out_shape=[
            jax.ShapeDtypeStruct((part, out_width), BF16),
            jax.ShapeDtypeStruct((part,), F32),
        ],
        scratch_shapes=[pltpu.VMEM((part,), F32), dma((2,))],
        compiler_params=pltpu.CompilerParams(vmem_limit_bytes=4 * 2**20),
    )(mixed, weight)


def solution(mesh):
    return jax.shard_map(
        per_device,
        mesh=mesh,
        in_specs=(
            P("dp", None),
            P(None, "dp"),
            P("dp"),
            P(),
            P("dp"),
            P(),
            P(None, "seq"),
            P(None, "seq"),
            P(None, "seq"),
            P("seq"),
            P("seq"),
            P("seq"),
            P("seq", None),
        ),
        out_specs=(P(("dp", "seq"), None), P(("dp", "seq"))),
        check_vma=False,
    )
```
